64 devices in a mesh: dp: 4 (over x, y), tp: 16 (over z, core).
Axes of the slice: x: 2, y: 2, z: 8, core: 2. Of those that a mesh axis runs over, the one named last changes fastest.
The devices are a block of a 4x4x8 slice.
Arguments:
- x: bfloat16 [256, 3072], P('dp'), parts along dimension 0
- k_cache: bfloat16 [256, 1024, 16, 256], P('dp', None, 'tp'), parts along dimension 0
- v_cache: bfloat16 [256, 1024, 16, 256], P('dp', None, 'tp'), parts along dimension 0
- gain_a: bfloat16 [3072], replicated
- wq: bfloat16 [3072, 4096], P(None, 'tp')
- wo: bfloat16 [4096, 3072], P('tp')
- gain_m: bfloat16 [3072], replicated
- w_gate: bfloat16 [3072, 24576], P(None, 'tp')
- w_up: bfloat16 [3072, 24576], P(None, 'tp')
- w_down: bfloat16 [24576, 3072], P('tp')
Outputs:
- output: bfloat16 [256, 3072], P('dp'), parts along dimension 0
There are 4 independent parts. The reference program is written for one: setup_inputs(seed, part) draws one part's arguments, and reference() takes and returns one part's arrays. A program takes and returns all parts, laid end to end along the dimension named above; an argument that names none is the same for every part.
All inputs are finite; a program needn't handle non-finite values.
Results may differ from the reference program's by a relative error of at most 0.017.
Values are sent between devices in bfloat16 or wider.
A program may use at most 768 MiB of HBM per device.

```python
import jax
import jax.numpy as jnp
from jax import lax

BATCH = 64
CACHE = 1024
D = 3072
HEADS = 16
KV_HEADS = 16
HEAD = 256
FF = 24576
THETA = 10000


def setup_inputs(seed: int = 0, part: int = 0) -> dict:
    kx, kc, kw, kn, kq, ko, km, kg, ku, kd = jax.random.split(jax.random.key(seed), 10)
    kx, kc, kw = (jax.random.fold_in(k, part) for k in (kx, kc, kw))

    def weights(key, rows, columns):
        return jax.random.normal(key, (rows, columns), jnp.float32) * rows**-0.5

    drawn = {
        "x": jax.random.normal(kx, (BATCH, D), jnp.float32),
        "k_cache": 2 * jax.random.normal(kc, (BATCH, CACHE, KV_HEADS, HEAD), jnp.float32),
        "v_cache": 4 * jax.random.normal(kw, (BATCH, CACHE, KV_HEADS, HEAD), jnp.float32),
        "gain_a": 1 + 0.1 * jax.random.normal(kn, (D,), jnp.float32),
        "wq": 2 * weights(kq, D, HEADS * HEAD),
        "wo": weights(ko, HEADS * HEAD, D),
        "gain_m": 1 + 0.1 * jax.random.normal(km, (D,), jnp.float32),
        "w_gate": weights(kg, D, FF),
        "w_up": weights(ku, D, FF),
        "w_down": 2 * weights(kd, FF, D),
    }
    return {k: v.astype(jnp.bfloat16) for k, v in drawn.items()}


def normed(x, gain):
    wide = x.astype(jnp.float32)
    scale = lax.rsqrt(jnp.mean(wide * wide, -1, keepdims=True) + 1e-6)
    return (wide * scale * gain.astype(jnp.float32)).astype(jnp.bfloat16)


def turned(t, place, theta):
    half = t.shape[-1] // 2
    angle = place.astype(jnp.float32)[:, None] * theta ** (-jnp.arange(half, dtype=jnp.float32) / half)
    cos, sin = jnp.cos(angle)[:, None], jnp.sin(angle)[:, None]
    a, b = t[..., :half].astype(jnp.float32), t[..., half:].astype(jnp.float32)
    return jnp.concatenate([a * cos - b * sin, b * cos + a * sin], -1).astype(jnp.bfloat16)


def matmul(a, w):
    return jnp.dot(a, w, preferred_element_type=jnp.float32).astype(jnp.bfloat16)


def einsum(form, a, b):
    return jnp.einsum(form, a.astype(jnp.float32), b.astype(jnp.float32))


def seen_by(a, wq, k_cache, v_cache, head, theta):
    batch, cache, kv_heads = k_cache.shape[:3]
    place = jnp.full((batch,), cache - 1)
    q = turned(matmul(a, wq).reshape(batch, -1, head), place, theta).reshape(batch, kv_heads, -1, head)
    scores = einsum("bgsd,bugd->bgsu", q, k_cache) * head**-0.5
    weights = jax.nn.softmax(scores, -1).astype(jnp.bfloat16)
    return einsum("bgsu,bugd->bgsd", weights, v_cache).astype(jnp.bfloat16).reshape(batch, -1)


def hidden_of(b, w_gate, w_up):
    gate = jnp.dot(b, w_gate, preferred_element_type=jnp.float32)
    up = jnp.dot(b, w_up, preferred_element_type=jnp.float32)
    return (jax.nn.silu(gate) * up).astype(jnp.bfloat16)


def reference(x, k_cache, v_cache, gain_a, wq, wo, gain_m, w_gate, w_up, w_down):
    seen = seen_by(normed(x, gain_a), wq, k_cache, v_cache, HEAD, THETA)
    h = (x.astype(jnp.float32) + jnp.dot(seen, wo, preferred_element_type=jnp.float32)).astype(jnp.bfloat16)
    hidden = hidden_of(normed(h, gain_m), w_gate, w_up)
    return (h.astype(jnp.float32) + jnp.dot(hidden, w_down, preferred_element_type=jnp.float32)).astype(jnp.bfloat16)
```

```python
import functools

import jax
import jax.numpy as jnp
import numpy as np
from jax import lax
from jax.experimental import pallas as pl
from jax.experimental.pallas import tpu as pltpu
from jax.sharding import PartitionSpec as P

HEAD = 256
THETA = 10000
CORES = 2
GROUP = 8
CHUNK = 16
SLOTS = 3
MESH = pl.DeviceIdType.MESH
F32, BF16 = jnp.float32, jnp.bfloat16


def rotary_table(cache, half):
    angle = np.float32(cache - 1) * (np.float32(THETA) ** (-np.arange(half, dtype=np.float32) / half))
    return np.stack([np.cos(angle), np.sin(angle)]).astype(np.float32)


def layer(n, x_hbm, k_hbm, v_hbm, ga_ref, trig_ref, wq_hbm, wo_hbm, gm_ref, wg_hbm, wu_hbm, wd_hbm, out_ref,
          x16, xs, a16, wq, wo, wg, wu, wd, kbuf, vbuf, q32, s32, hb,
          send1, recv1, hg, send2, recv2, yg,
          in_sem, k_sem, v_sem, s1s, s1r, g1s, g1r, s2s, s2r, g2s, g2r):
    rows, d = x16.shape
    ff = wg.shape[1]
    groups, chunks = rows // GROUP, rows // CHUNK
    half = CHUNK // CORES
    chips = n // CORES
    cols = d // chips
    me = lax.axis_index("tp")
    z, core = me // CORES, lax.rem(me, CORES)
    tiles = d // 128

    def peer(i):
        return lax.rem(me + i, n)

    order = sorted(range(1, n), key=lambda i: -min(i, n - i))

    load_x = pltpu.make_async_copy(x_hbm, x16, in_sem.at[0])
    load_wq = pltpu.make_async_copy(wq_hbm, wq, in_sem.at[1])
    load_wo = pltpu.make_async_copy(wo_hbm, wo, in_sem.at[2])
    load_wg = pltpu.make_async_copy(wg_hbm, wg, in_sem.at[3])
    load_wu = pltpu.make_async_copy(wu_hbm, wu, in_sem.at[4])
    load_wd = pltpu.make_async_copy(wd_hbm, wd, in_sem.at[5])

    def load_k(g):
        slot = lax.rem(g, SLOTS)
        return pltpu.make_async_copy(k_hbm.at[pl.ds(g * GROUP, GROUP)], kbuf.at[slot], k_sem.at[slot])

    def load_v(g):
        slot = lax.rem(g, SLOTS)
        return pltpu.make_async_copy(v_hbm.at[pl.ds(g * GROUP, GROUP)], vbuf.at[slot], v_sem.at[slot])

    load_x.start()
    load_wq.start()
    for g in range(SLOTS):
        load_k(g).start()
        load_v(g).start()
        if g == 0:
            load_wo.start()

    barrier = pltpu.get_barrier_semaphore()
    for i in range(1, n):
        pl.semaphore_signal(barrier, inc=1, device_id={"tp": peer(i)}, device_id_type=MESH)

    load_x.wait()
    part = jnp.zeros((rows, 128), F32)
    for j in range(tiles):
        block = x16[:, pl.ds(128 * j, 128)].astype(F32)
        xs[:, pl.ds(128 * j, 128)] = block
        part += block * block
    scale = lax.rsqrt(jnp.sum(part, -1, keepdims=True) / d + 1e-6)
    gain = ga_ref[...].astype(F32)
    for j in range(tiles):
        a16[:, pl.ds(128 * j, 128)] = (xs[:, pl.ds(128 * j, 128)] * scale * gain[j:j + 1]).astype(BF16)
    load_wq.wait()
    q = jnp.dot(a16[...], wq[...], preferred_element_type=F32).astype(BF16).astype(F32)
    turn = HEAD // 2
    cos, sin = trig_ref[0:1], trig_ref[1:2]
    qa, qb = q[:, :turn], q[:, turn:]
    q32[:, :turn] = (qa * cos - qb * sin).astype(BF16).astype(F32)
    q32[:, turn:] = (qb * cos + qa * sin).astype(BF16).astype(F32)

    pl.semaphore_wait(barrier, n - 1)

    def piece(src, dst, ssem, rsem, to):
        return pltpu.make_async_remote_copy(src_ref=src, dst_ref=dst, send_sem=ssem, recv_sem=rsem,
                                            device_id={"tp": to}, device_id_type=MESH)

    def scatter1(c):
        seen = s32[pl.ds(pl.multiple_of(c * CHUNK, CHUNK), CHUNK), :].astype(BF16)
        for t in range(chips):
            term = jnp.dot(seen, wo[:, pl.ds(t * cols, cols)], preferred_element_type=F32)
            for k in range(CORES):
                send1[c, CORES * t + k] = term[half * k:half * (k + 1)].astype(BF16)
        for i in order:
            to = peer(i)
            piece(send1.at[c, to], recv1.at[c, me], s1s.at[c, to], s1r.at[c, me], to).start()

    def gather1(c):
        total = send1[c, me].astype(F32)
        for i in order:
            frm = peer(i)
            piece(send1.at[c, frm], recv1.at[c, frm], s1s.at[c, frm], s1r.at[c, frm], frm).wait_recv()
        for i in order:
            total += recv1[c, peer(i)].astype(F32)
        at = pl.ds(pl.multiple_of(c * CHUNK + core * half, half), half)
        hg[c, me] = (xs[at, pl.ds(pl.multiple_of(z * cols, 128), cols)] + total).astype(BF16)
        for i in order:
            to = peer(i)
            piece(hg.at[c, me], hg.at[c, me], g1s.at[c, to], g1r.at[c, me], to).start()

    line = lax.broadcasted_iota(jnp.int32, (GROUP, 1), 0)

    def attend(g, _):
        slot = lax.rem(g, SLOTS)
        at = pl.ds(pl.multiple_of(g * GROUP, GROUP), GROUP)
        load_k(g).wait()
        qg = q32[at, :]
        scores = None
        for i in range(GROUP):
            mine = jnp.where(line == i, qg, 0.0).astype(BF16)
            s = lax.dot_general(mine, kbuf[slot, i], (((1,), (1,)), ((), ())), preferred_element_type=F32)
            scores = s if scores is None else scores + s

        @pl.when(g + SLOTS < groups)
        def _():
            load_k(g + SLOTS).start()

        scores = scores * HEAD**-0.5
        e = jnp.exp(scores - jnp.max(scores, -1, keepdims=True))
        w = e * (1.0 / jnp.sum(e, -1, keepdims=True))
        load_v(g).wait()
        seen = None
        for i in range(GROUP):
            mine = jnp.where(line == i, w, 0.0).astype(BF16)
            s = jnp.dot(mine, vbuf[slot, i], preferred_element_type=F32)
            seen = s if seen is None else seen + s
        s32[at, :] = seen

        @pl.when(g + SLOTS < groups)
        def _():
            load_v(g + SLOTS).start()

        @pl.when(g == groups - SLOTS - 1)
        def _():
            load_wg.start()
            load_wu.start()
            load_wd.start()

        @pl.when(g == 1)
        def _():
            load_wo.wait()

        per = CHUNK // GROUP

        @pl.when(lax.rem(g, per) == per - 1)
        def _():
            scatter1(g // per)

        @pl.when((lax.rem(g, per) == 0) & (g >= 2 * per))
        def _():
            gather1(g // per - 2)

        return 0

    lax.fori_loop(0, groups, attend, 0)
    for c in range(max(0, groups // (CHUNK // GROUP) - 2), chunks):
        gather1(c)

    gain_m = gm_ref[...].astype(F32)
    for c in range(chunks):
        for i in order:
            frm = peer(i)
            piece(hg.at[c, frm], hg.at[c, frm], g1s.at[c, frm], g1r.at[c, frm], frm).wait_recv()
        blocks = []
        part = jnp.zeros((CHUNK, 128), F32)
        for t in range(chips):
            block = jnp.concatenate([hg[c, CORES * t + k].astype(F32) for k in range(CORES)], 0)
            for u in range(cols // 128):
                sub = block[:, 128 * u:128 * (u + 1)]
                blocks.append(sub)
                part += sub * sub
        scale = lax.rsqrt(jnp.sum(part, -1, keepdims=True) / d + 1e-6)
        for j in range(tiles):
            a16[pl.ds(c * CHUNK, CHUNK), pl.ds(128 * j, 128)] = (blocks[j] * scale * gain_m[j:j + 1]).astype(BF16)

    load_wg.wait()
    load_wu.wait()
    width = 256

    def hidden(j, _):
        at = pl.ds(pl.multiple_of(j * width, width), width)
        b = a16[...]
        gate = jnp.dot(b, wg[:, at], preferred_element_type=F32)
        up = jnp.dot(b, wu[:, at], preferred_element_type=F32)
        hb[:, at] = (gate / (1.0 + jnp.exp(-gate)) * up).astype(BF16)
        return 0

    lax.fori_loop(0, ff // width, hidden, 0)
    load_wd.wait()

    far = [chips // 2]
    for i in range(chips // 2 - 1, 0, -1):
        far += [i, chips - i]
    far.append(0)

    for i in far:
        t = lax.rem(z + i, chips)
        term = jnp.dot(hb[...], wd[:, pl.ds(pl.multiple_of(t * cols, 128), cols)], preferred_element_type=F32)
        for k in range(CORES):
            to = CORES * t + k
            for c in range(chunks):
                send2[to, c] = term[c * CHUNK + half * k:c * CHUNK + half * (k + 1)].astype(BF16)
            if i:
                piece(send2.at[to], recv2.at[me], s2s.at[to], s2r.at[me], to).start()
    other = CORES * z + (CORES - 1 - core)
    piece(send2.at[other], recv2.at[me], s2s.at[other], s2r.at[me], other).start()

    for i in order:
        frm = peer(i)
        piece(send2.at[frm], recv2.at[frm], s2s.at[frm], s2r.at[frm], frm).wait_recv()
    for c in range(chunks):
        total = send2[me, c].astype(F32)
        for i in order:
            total += recv2[peer(i), c].astype(F32)
        yg[me, c] = (hg[c, me].astype(F32) + total).astype(BF16)
    for i in order:
        to = peer(i)
        piece(yg.at[me], yg.at[me], g2s.at[to], g2r.at[me], to).start()
    for i in order:
        frm = peer(i)
        piece(yg.at[frm], yg.at[frm], g2s.at[frm], g2r.at[frm], frm).wait_recv()
    for c in range(chunks):
        for t in range(chips):
            both = jnp.concatenate([yg[CORES * t + k, c].astype(F32) for k in range(CORES)], 0)
            out_ref[pl.ds(c * CHUNK, CHUNK), pl.ds(t * cols, cols)] = both.astype(BF16)

    for i in order:
        to = peer(i)
        for c in range(chunks):
            piece(send1.at[c, to], recv1.at[c, me], s1s.at[c, to], s1r.at[c, me], to).wait_send()
            piece(hg.at[c, me], hg.at[c, me], g1s.at[c, to], g1r.at[c, me], to).wait_send()
        piece(send2.at[to], recv2.at[me], s2s.at[to], s2r.at[me], to).wait_send()
        piece(yg.at[me], yg.at[me], g2s.at[to], g2r.at[me], to).wait_send()


def solution(mesh):
    n = mesh.shape["tp"]

    def step(x, k_cache, v_cache, gain_a, wq, wo, gain_m, w_gate, w_up, w_down):
        rows, d = x.shape
        cache = k_cache.shape[1]
        ff = w_gate.shape[1]
        k_cache, v_cache = k_cache.reshape(rows, cache, HEAD), v_cache.reshape(rows, cache, HEAD)
        chunks, half, cols = rows // CHUNK, CHUNK // CORES, d // (n // CORES)
        trig = jnp.asarray(rotary_table(cache, HEAD // 2))
        any_, vmem = pl.BlockSpec(memory_space=pl.ANY), pl.BlockSpec(memory_space=pltpu.VMEM)
        dma = pltpu.SemaphoreType.DMA
        return pl.pallas_call(
            functools.partial(layer, n),
            name="layer",
            out_shape=jax.ShapeDtypeStruct((rows, d), BF16),
            in_specs=[any_, any_, any_, vmem, vmem, any_, any_, vmem, any_, any_, any_],
            out_specs=vmem,
            scratch_shapes=[
                pltpu.VMEM((rows, d), BF16),
                pltpu.VMEM((rows, d), F32),
                pltpu.VMEM((rows, d), BF16),
                pltpu.VMEM(wq.shape, BF16),
                pltpu.VMEM(wo.shape, BF16),
                pltpu.VMEM(w_gate.shape, BF16),
                pltpu.VMEM(w_up.shape, BF16),
                pltpu.VMEM(w_down.shape, BF16),
                pltpu.VMEM((SLOTS, GROUP, cache, HEAD), BF16),
                pltpu.VMEM((SLOTS, GROUP, cache, HEAD), BF16),
                pltpu.VMEM((rows, HEAD), F32),
                pltpu.VMEM((rows, HEAD), F32),
                pltpu.VMEM((rows, ff), BF16),
                pltpu.VMEM((chunks, n, half, cols), BF16),
                pltpu.VMEM((chunks, n, half, cols), BF16),
                pltpu.VMEM((chunks, n, half, cols), BF16),
                pltpu.VMEM((n, chunks, half, cols), BF16),
                pltpu.VMEM((n, chunks, half, cols), BF16),
                pltpu.VMEM((n, chunks, half, cols), BF16),
                dma((6,)),
                dma((SLOTS,)),
                dma((SLOTS,)),
                dma((chunks, n)),
                dma((chunks, n)),
                dma((chunks, n)),
                dma((chunks, n)),
                dma((n,)),
                dma((n,)),
                dma((n,)),
                dma((n,)),
            ],
            compiler_params=pltpu.CompilerParams(
                collective_id=0, has_side_effects=True, vmem_limit_bytes=67_043_328
            ),
        )(x, k_cache, v_cache, gain_a.reshape(-1, 128), trig, wq, wo, gain_m.reshape(-1, 128), w_gate, w_up, w_down)

    states, cache, columns, rows_of = P("dp", None), P("dp", None, "tp", None), P(None, "tp"), P("tp", None)
    return jax.shard_map(
        step,
        mesh=mesh,
        in_specs=(states, cache, cache, P(None), columns, rows_of, P(None), columns, columns, rows_of),
        out_specs=states,
        check_vma=False,
    )
```

```python
import functools

import jax
import jax.numpy as jnp
import numpy as np
from jax import lax
from jax.experimental import pallas as pl
from jax.experimental.pallas import tpu as pltpu
from jax.sharding import PartitionSpec as P

HEAD = 256
THETA = 10000
CORES = 2
GROUP = 8
CHUNK = 16
SLOTS = 3
MESH = pl.DeviceIdType.MESH
F32, BF16 = jnp.float32, jnp.bfloat16


def rotary_table(cache, half):
    angle = np.float32(cache - 1) * (np.float32(THETA) ** (-np.arange(half, dtype=np.float32) / half))
    return np.stack([np.cos(angle), np.sin(angle)]).astype(np.float32)


def layer(n, x_hbm, k_hbm, v_hbm, ga_ref, trig_ref, wq_hbm, wo_hbm, gm_ref, wg_hbm, wu_hbm, wd_hbm, out_ref,
          x16, xs, a16, wq, wo, wg, wu, wd, kbuf, vbuf, q32, s32, hb,
          send1, recv1, hg, send2, recv2, yg,
          in_sem, k_sem, v_sem, s1s, s1r, g1s, g1r, s2s, s2r, g2s, g2r):
    rows, d = x16.shape
    ff = wg.shape[1]
    groups, chunks = rows // GROUP, rows // CHUNK
    half = CHUNK // CORES
    chips = n // CORES
    cols = d // chips
    me = lax.axis_index("tp")
    z, core = me // CORES, lax.rem(me, CORES)
    tiles = d // 128

    def peer(i):
        return lax.rem(me + i, n)

    order = sorted(range(1, n), key=lambda i: -min(i, n - i))

    load_x = pltpu.make_async_copy(x_hbm, x16, in_sem.at[0])
    load_wq = pltpu.make_async_copy(wq_hbm, wq, in_sem.at[1])
    load_wo = pltpu.make_async_copy(wo_hbm, wo, in_sem.at[2])
    load_wg = pltpu.make_async_copy(wg_hbm, wg, in_sem.at[3])
    load_wu = pltpu.make_async_copy(wu_hbm, wu, in_sem.at[4])
    load_wd = pltpu.make_async_copy(wd_hbm, wd, in_sem.at[5])

    def load_k(g):
        slot = lax.rem(g, SLOTS)
        return pltpu.make_async_copy(k_hbm.at[pl.ds(g * GROUP, GROUP)], kbuf.at[slot], k_sem.at[slot])

    def load_v(g):
        slot = lax.rem(g, SLOTS)
        return pltpu.make_async_copy(v_hbm.at[pl.ds(g * GROUP, GROUP)], vbuf.at[slot], v_sem.at[slot])

    load_x.start()
    load_wq.start()
    for g in range(SLOTS):
        load_k(g).start()
        load_v(g).start()
        if g == 0:
            load_wo.start()

    barrier = pltpu.get_barrier_semaphore()
    for i in range(1, n):
        pl.semaphore_signal(barrier, inc=1, device_id={"tp": peer(i)}, device_id_type=MESH)

    load_x.wait()
    part = jnp.zeros((rows, 128), F32)
    for j in range(tiles):
        block = x16[:, pl.ds(128 * j, 128)].astype(F32)
        xs[:, pl.ds(128 * j, 128)] = block
        part += block * block
    scale = lax.rsqrt(jnp.sum(part, -1, keepdims=True) / d + 1e-6)
    gain = ga_ref[...].astype(F32)
    for j in range(tiles):
        a16[:, pl.ds(128 * j, 128)] = (xs[:, pl.ds(128 * j, 128)] * scale * gain[j:j + 1]).astype(BF16)
    load_wq.wait()
    q = jnp.dot(a16[...], wq[...], preferred_element_type=F32).astype(BF16).astype(F32)
    turn = HEAD // 2
    cos, sin = trig_ref[0:1], trig_ref[1:2]
    qa, qb = q[:, :turn], q[:, turn:]
    q32[:, :turn] = (qa * cos - qb * sin).astype(BF16).astype(F32)
    q32[:, turn:] = (qb * cos + qa * sin).astype(BF16).astype(F32)

    pl.semaphore_wait(barrier, n - 1)

    def piece(src, dst, ssem, rsem, to):
        return pltpu.make_async_remote_copy(src_ref=src, dst_ref=dst, send_sem=ssem, recv_sem=rsem,
                                            device_id={"tp": to}, device_id_type=MESH)

    def scatter1(c):
        seen = s32[pl.ds(pl.multiple_of(c * CHUNK, CHUNK), CHUNK), :].astype(BF16)
        for t in range(chips):
            term = jnp.dot(seen, wo[:, pl.ds(t * cols, cols)], preferred_element_type=F32)
            for k in range(CORES):
                send1[c, CORES * t + k] = term[half * k:half * (k + 1)].astype(BF16)
        for i in order:
            to = peer(i)
            piece(send1.at[c, to], recv1.at[c, me], s1s.at[c, to], s1r.at[c, me], to).start()

    def gather1(c):
        total = send1[c, me].astype(F32)
        for i in order:
            frm = peer(i)
            piece(send1.at[c, frm], recv1.at[c, frm], s1s.at[c, frm], s1r.at[c, frm], frm).wait_recv()
        for i in order:
            total += recv1[c, peer(i)].astype(F32)
        at = pl.ds(pl.multiple_of(c * CHUNK + core * half, half), half)
        hg[c, me] = (xs[at, pl.ds(pl.multiple_of(z * cols, 128), cols)] + total).astype(BF16)
        for i in order:
            to = peer(i)
            piece(hg.at[c, me], hg.at[c, me], g1s.at[c, to], g1r.at[c, me], to).start()

    line = lax.broadcasted_iota(jnp.int32, (GROUP, 1), 0)

    def attend(g, _):
        slot = lax.rem(g, SLOTS)
        at = pl.ds(pl.multiple_of(g * GROUP, GROUP), GROUP)
        load_k(g).wait()
        qg = q32[at, :]
        lhs = [jnp.where(line == i, qg, 0.0).astype(BF16) for i in range(GROUP)]
        scores = []
        for j in range(kbuf.shape[2] // 256):
            total = None
            for i in range(GROUP):
                s = lax.dot_general(lhs[i], kbuf[slot, i, pl.ds(256 * j, 256)], (((1,), (1,)), ((), ())), preferred_element_type=F32)
                total = s if total is None else total + s
            scores.append(total)
        scores = jnp.concatenate(scores, 1)

        @pl.when(g + SLOTS < groups)
        def _():
            load_k(g + SLOTS).start()

        scores = scores * HEAD**-0.5
        e = jnp.exp(scores - jnp.max(scores, -1, keepdims=True))
        w = e * (1.0 / jnp.sum(e, -1, keepdims=True))
        load_v(g).wait()
        lhs = [jnp.where(line == i, w, 0.0).astype(BF16) for i in range(GROUP)]
        for j in range(HEAD // 128):
            total = None
            for i in range(GROUP):
                s = jnp.dot(lhs[i], vbuf[slot, i, :, pl.ds(128 * j, 128)], preferred_element_type=F32)
                total = s if total is None else total + s
            s32[at, pl.ds(128 * j, 128)] = total

        @pl.when(g + SLOTS < groups)
        def _():
            load_v(g + SLOTS).start()

        @pl.when(g == groups - SLOTS - 1)
        def _():
            load_wg.start()
            load_wu.start()
            load_wd.start()

        @pl.when(g == 1)
        def _():
            load_wo.wait()

        per = CHUNK // GROUP

        @pl.when(lax.rem(g, per) == per - 1)
        def _():
            scatter1(g // per)

        @pl.when((lax.rem(g, per) == 0) & (g >= 2 * per))
        def _():
            gather1(g // per - 2)

        return 0

    lax.fori_loop(0, groups, attend, 0)
    for c in range(max(0, groups // (CHUNK // GROUP) - 2), chunks):
        gather1(c)

    gain_m = gm_ref[...].astype(F32)
    for c in range(chunks):
        for i in order:
            frm = peer(i)
            piece(hg.at[c, frm], hg.at[c, frm], g1s.at[c, frm], g1r.at[c, frm], frm).wait_recv()
        blocks = []
        part = jnp.zeros((CHUNK, 128), F32)
        for t in range(chips):
            block = jnp.concatenate([hg[c, CORES * t + k].astype(F32) for k in range(CORES)], 0)
            for u in range(cols // 128):
                sub = block[:, 128 * u:128 * (u + 1)]
                blocks.append(sub)
                part += sub * sub
        scale = lax.rsqrt(jnp.sum(part, -1, keepdims=True) / d + 1e-6)
        for j in range(tiles):
            a16[pl.ds(c * CHUNK, CHUNK), pl.ds(128 * j, 128)] = (blocks[j] * scale * gain_m[j:j + 1]).astype(BF16)

    load_wg.wait()
    load_wu.wait()
    width = 256

    def hidden(j, _):
        at = pl.ds(pl.multiple_of(j * width, width), width)
        b = a16[...]
        gate = jnp.dot(b, wg[:, at], preferred_element_type=F32)
        up = jnp.dot(b, wu[:, at], preferred_element_type=F32)
        hb[:, at] = (gate / (1.0 + jnp.exp(-gate)) * up).astype(BF16)
        return 0

    lax.fori_loop(0, ff // width, hidden, 0, unroll=2)
    load_wd.wait()

    pair = 2 * cols
    pairs = chips // 2
    for i in (pairs // 2, pairs // 2 - 1, pairs - 1, 0):
        p = lax.rem(z // 2 + i, pairs)
        b = hb[...]
        terms = []
        for u in range(pair // width):
            at = pl.ds(pl.multiple_of(p * pair + u * width, width), width)
            terms.append(jnp.dot(b, wd[:, at], preferred_element_type=F32))
        term = jnp.concatenate(terms, 1)
        for t in range(2):
            for k in range(CORES):
                for c in range(chunks):
                    row = c * CHUNK + half * k
                    send2[2 * CORES * p + CORES * t + k, c] = term[row:row + half, t * cols:(t + 1) * cols].astype(BF16)
        for t in range(2 * CORES):
            to = 2 * CORES * p + t

            @pl.when(to != me)
            def _():
                piece(send2.at[to], recv2.at[me], s2s.at[to], s2r.at[me], to).start()
    for i in order:
        frm = peer(i)
        piece(send2.at[frm], recv2.at[frm], s2s.at[frm], s2r.at[frm], frm).wait_recv()
    for c in range(chunks):
        total = send2[me, c].astype(F32)
        for i in order:
            total += recv2[peer(i), c].astype(F32)
        yg[me, c] = (hg[c, me].astype(F32) + total).astype(BF16)
    for i in order:
        to = peer(i)
        piece(yg.at[me], yg.at[me], g2s.at[to], g2r.at[me], to).start()
    for i in order:
        frm = peer(i)
        piece(yg.at[frm], yg.at[frm], g2s.at[frm], g2r.at[frm], frm).wait_recv()
    for c in range(chunks):
        for t in range(chips):
            both = jnp.concatenate([yg[CORES * t + k, c].astype(F32) for k in range(CORES)], 0)
            out_ref[pl.ds(c * CHUNK, CHUNK), pl.ds(t * cols, cols)] = both.astype(BF16)

    for i in order:
        to = peer(i)
        for c in range(chunks):
            piece(send1.at[c, to], recv1.at[c, me], s1s.at[c, to], s1r.at[c, me], to).wait_send()
            piece(hg.at[c, me], hg.at[c, me], g1s.at[c, to], g1r.at[c, me], to).wait_send()
        piece(send2.at[to], recv2.at[me], s2s.at[to], s2r.at[me], to).wait_send()
        piece(yg.at[me], yg.at[me], g2s.at[to], g2r.at[me], to).wait_send()


def solution(mesh):
    n = mesh.shape["tp"]

    def step(x, k_cache, v_cache, gain_a, wq, wo, gain_m, w_gate, w_up, w_down):
        rows, d = x.shape
        cache = k_cache.shape[1]
        ff = w_gate.shape[1]
        k_cache, v_cache = k_cache.reshape(rows, cache, HEAD), v_cache.reshape(rows, cache, HEAD)
        chunks, half, cols = rows // CHUNK, CHUNK // CORES, d // (n // CORES)
        trig = jnp.asarray(rotary_table(cache, HEAD // 2))
        any_, vmem = pl.BlockSpec(memory_space=pl.ANY), pl.BlockSpec(memory_space=pltpu.VMEM)
        dma = pltpu.SemaphoreType.DMA
        return pl.pallas_call(
            functools.partial(layer, n),
            name="layer",
            out_shape=jax.ShapeDtypeStruct((rows, d), BF16),
            in_specs=[any_, any_, any_, vmem, vmem, any_, any_, vmem, any_, any_, any_],
            out_specs=vmem,
            scratch_shapes=[
                pltpu.VMEM((rows, d), BF16),
                pltpu.VMEM((rows, d), F32),
                pltpu.VMEM((rows, d), BF16),
                pltpu.VMEM(wq.shape, BF16),
                pltpu.VMEM(wo.shape, BF16),
                pltpu.VMEM(w_gate.shape, BF16),
                pltpu.VMEM(w_up.shape, BF16),
                pltpu.VMEM(w_down.shape, BF16),
                pltpu.VMEM((SLOTS, GROUP, cache, HEAD), BF16),
                pltpu.VMEM((SLOTS, GROUP, cache, HEAD), BF16),
                pltpu.VMEM((rows, HEAD), F32),
                pltpu.VMEM((rows, HEAD), F32),
                pltpu.VMEM((rows, ff), BF16),
                pltpu.VMEM((chunks, n, half, cols), BF16),
                pltpu.VMEM((chunks, n, half, cols), BF16),
                pltpu.VMEM((chunks, n, half, cols), BF16),
                pltpu.VMEM((n, chunks, half, cols), BF16),
                pltpu.VMEM((n, chunks, half, cols), BF16),
                pltpu.VMEM((n, chunks, half, cols), BF16),
                dma((6,)),
                dma((SLOTS,)),
                dma((SLOTS,)),
                dma((chunks, n)),
                dma((chunks, n)),
                dma((chunks, n)),
                dma((chunks, n)),
                dma((n,)),
                dma((n,)),
                dma((n,)),
                dma((n,)),
            ],
            compiler_params=pltpu.CompilerParams(
                collective_id=0, has_side_effects=True, vmem_limit_bytes=67_043_328
            ),
        )(x, k_cache, v_cache, gain_a.reshape(-1, 128), trig, wq, wo, gain_m.reshape(-1, 128), w_gate, w_up, w_down)

    states, cache, columns, rows_of = P("dp", None), P("dp", None, "tp", None), P(None, "tp"), P("tp", None)
    return jax.shard_map(
        step,
        mesh=mesh,
        in_specs=(states, cache, cache, P(None), columns, rows_of, P(None), columns, columns, rows_of),
        out_specs=states,
        check_vma=False,
    )
```

```python
import functools

import jax
import jax.numpy as jnp
import numpy as np
from jax import lax
from jax.experimental import pallas as pl
from jax.experimental.pallas import tpu as pltpu
from jax.sharding import PartitionSpec as P

HEAD = 256
THETA = 10000
CORES = 2
GROUP = 8
CHUNK = 16
SLOTS = 3
LATE = 1
UNROLL = 2
MESH = pl.DeviceIdType.MESH
F32, BF16 = jnp.float32, jnp.bfloat16


def rotary_table(cache, half):
    angle = np.float32(cache - 1) * (np.float32(THETA) ** (-np.arange(half, dtype=np.float32) / half))
    return np.stack([np.cos(angle), np.sin(angle)]).astype(np.float32)


def layer(n, x_hbm, k_hbm, v_hbm, ga_ref, trig_ref, wq_hbm, wo_hbm, gm_ref, wg_hbm, wu_hbm, wd_hbm, out_ref,
          x16, xs, a16, wq, wo, wg, wu, wd, kbuf, vbuf, q32, hb,
          send1, recv1, hg, send2, recv2, yg, send3, recv3, yh,
          in_sem, k_sem, v_sem, s1s, s1r, g1s, g1r, s2s, s2r, g2s, g2r):
    rows, d = x16.shape
    ff = wg.shape[1]
    groups, chunks = rows // GROUP, rows // CHUNK
    half = CHUNK // CORES
    chips = n // CORES
    cols = d // chips
    me = lax.axis_index("tp")
    z, core = me // CORES, lax.rem(me, CORES)
    tiles = d // 128

    def peer(i):
        return lax.rem(me + i, n)

    order = sorted(range(1, n), key=lambda i: -min(i, n - i))
    far = [chips // 2]
    for i in range(chips // 2 - 1, 0, -1):
        far += [i, chips - i]
    far.append(0)

    load_x = pltpu.make_async_copy(x_hbm, x16, in_sem.at[0])
    load_wq = pltpu.make_async_copy(wq_hbm, wq, in_sem.at[1])
    load_wo = pltpu.make_async_copy(wo_hbm, wo, in_sem.at[2])
    load_wg = pltpu.make_async_copy(wg_hbm, wg, in_sem.at[3])
    load_wu = pltpu.make_async_copy(wu_hbm, wu, in_sem.at[4])
    load_wd = pltpu.make_async_copy(wd_hbm, wd, in_sem.at[5])

    def load_k(g):
        slot = lax.rem(g, SLOTS)
        return pltpu.make_async_copy(k_hbm.at[pl.ds(g * GROUP, GROUP)], kbuf.at[slot], k_sem.at[slot])

    def load_v(g):
        slot = lax.rem(g, SLOTS)
        return pltpu.make_async_copy(v_hbm.at[pl.ds(g * GROUP, GROUP)], vbuf.at[slot], v_sem.at[slot])

    load_x.start()
    load_wq.start()
    for g in range(SLOTS):
        load_k(g).start()
        load_v(g).start()
        if g == 0:
            load_wo.start()

    barrier = pltpu.get_barrier_semaphore()
    for i in range(1, n):
        pl.semaphore_signal(barrier, inc=1, device_id={"tp": peer(i)}, device_id_type=MESH)

    load_x.wait()
    part = jnp.zeros((rows, 128), F32)
    for j in range(tiles):
        block = x16[:, pl.ds(128 * j, 128)].astype(F32)
        xs[:, pl.ds(128 * j, 128)] = block
        part += block * block
    scale = lax.rsqrt(jnp.sum(part, -1, keepdims=True) / d + 1e-6)
    gain = ga_ref[...].astype(F32)
    for j in range(tiles):
        a16[:, pl.ds(128 * j, 128)] = (xs[:, pl.ds(128 * j, 128)] * scale * gain[j:j + 1]).astype(BF16)
    load_wq.wait()
    q = jnp.dot(a16[...], wq[...], preferred_element_type=F32).astype(BF16).astype(F32)
    turn = HEAD // 2
    cos, sin = trig_ref[0:1], trig_ref[1:2]
    qa, qb = q[:, :turn], q[:, turn:]
    q32[:, :turn] = (qa * cos - qb * sin).astype(BF16).astype(F32)
    q32[:, turn:] = (qb * cos + qa * sin).astype(BF16).astype(F32)

    pl.semaphore_wait(barrier, n - 1)

    def piece(src, dst, ssem, rsem, to):
        return pltpu.make_async_remote_copy(src_ref=src, dst_ref=dst, send_sem=ssem, recv_sem=rsem,
                                            device_id={"tp": to}, device_id_type=MESH)

    def scatter1(u, seen):
        for t in range(chips):
            term = jnp.dot(seen, wo[:, pl.ds(t * cols, cols)], preferred_element_type=F32)
            send1[u, t] = term.astype(BF16)
        kind = lax.rem(u, CORES)
        c = u // CORES
        for i in far:
            t = lax.rem(z + i, chips)
            to = CORES * t + kind
            copy = piece(send1.at[u, t], recv1.at[c, me], s1s.at[u, t], s1r.at[c, me], to)
            if i:
                copy.start()
            else:
                pl.when(core != kind)(copy.start)

    def gather1(c):
        u = CORES * c + core
        total = send1[u, z].astype(F32)
        for i in order:
            frm = peer(i)
            piece(send1.at[u, z], recv1.at[c, frm], s1s.at[u, z], s1r.at[c, frm], frm).wait_recv()
        for i in order:
            total += recv1[c, peer(i)].astype(F32)
        at = pl.ds(pl.multiple_of(u * half, half), half)
        hg[c, me] = (xs[at, pl.ds(pl.multiple_of(z * cols, 128), cols)] + total).astype(BF16)
        for i in order:
            to = peer(i)
            piece(hg.at[c, me], hg.at[c, me], g1s.at[c, to], g1r.at[c, me], to).start()

    line = lax.broadcasted_iota(jnp.int32, (GROUP, 1), 0)

    def attend(g, _):
        slot = lax.rem(g, SLOTS)
        at = pl.ds(pl.multiple_of(g * GROUP, GROUP), GROUP)
        load_k(g).wait()
        qg = q32[at, :]
        lhs = [jnp.where(line == i, qg, 0.0).astype(BF16) for i in range(GROUP)]
        scores = []
        for j in range(kbuf.shape[2] // 256):
            total = None
            for i in range(GROUP):
                s = lax.dot_general(lhs[i], kbuf[slot, i, pl.ds(256 * j, 256)], (((1,), (1,)), ((), ())), preferred_element_type=F32)
                total = s if total is None else total + s
            scores.append(total)
        scores = jnp.concatenate(scores, 1)

        @pl.when(g + SLOTS < groups)
        def _():
            load_k(g + SLOTS).start()

        scores = scores * HEAD**-0.5
        e = jnp.exp(scores - jnp.max(scores, -1, keepdims=True))
        w = e * (1.0 / jnp.sum(e, -1, keepdims=True))
        load_v(g).wait()
        lhs = [jnp.where(line == i, w, 0.0).astype(BF16) for i in range(GROUP)]
        seen = []
        for j in range(HEAD // 128):
            total = None
            for i in range(GROUP):
                s = jnp.dot(lhs[i], vbuf[slot, i, :, pl.ds(128 * j, 128)], preferred_element_type=F32)
                total = s if total is None else total + s
            seen.append(total)
        seen = jnp.concatenate(seen, 1).astype(BF16)

        @pl.when(g + SLOTS < groups)
        def _():
            load_v(g + SLOTS).start()

        @pl.when(g == groups - SLOTS - 1)
        def _():
            load_wg.start()
            load_wu.start()
            load_wd.start()

        @pl.when(g == 0)
        def _():
            load_wo.wait()

        scatter1(g, seen)

        @pl.when((lax.rem(g, CORES) == 0) & (g >= 2 * CORES))
        def _():
            gather1(g // CORES - 2)

        return 0

    lax.fori_loop(0, groups, attend, 0)
    for c in range(chunks - 2, chunks):
        gather1(c)

    gain_m = gm_ref[...].astype(F32)
    width = 256
    pair = 2 * cols
    pairs = chips // 2

    def mlp(first, count, send, recv, ssem, rsem):
        for c in range(first, first + count):
            for i in order:
                frm = peer(i)
                piece(hg.at[c, frm], hg.at[c, frm], g1s.at[c, frm], g1r.at[c, frm], frm).wait_recv()
            blocks = []
            part = jnp.zeros((CHUNK, 128), F32)
            for t in range(chips):
                block = jnp.concatenate([hg[c, CORES * t + k].astype(F32) for k in range(CORES)], 0)
                for u in range(cols // 128):
                    sub = block[:, 128 * u:128 * (u + 1)]
                    blocks.append(sub)
                    part += sub * sub
            scale = lax.rsqrt(jnp.sum(part, -1, keepdims=True) / d + 1e-6)
            for j in range(tiles):
                a16[pl.ds(c * CHUNK, CHUNK), pl.ds(128 * j, 128)] = (blocks[j] * scale * gain_m[j:j + 1]).astype(BF16)

        mine = pl.ds(first * CHUNK, count * CHUNK)
        if first == 0:
            load_wg.wait()
            load_wu.wait()

        def hidden(j, _):
            at = pl.ds(pl.multiple_of(j * width, width), width)
            b = a16[mine, :]
            gate = jnp.dot(b, wg[:, at], preferred_element_type=F32)
            up = jnp.dot(b, wu[:, at], preferred_element_type=F32)
            hb[mine, at] = (gate / (1.0 + jnp.exp(-gate)) * up).astype(BF16)
            return 0

        lax.fori_loop(0, ff // width, hidden, 0, unroll=UNROLL)
        if first == 0:
            load_wd.wait()

        for i in (pairs // 2, pairs // 2 - 1, pairs - 1, 0):
            p = lax.rem(z // 2 + i, pairs)
            b = hb[mine, :]
            terms = []
            for o in range(0, pair, width):
                at = pl.ds(pl.multiple_of(p * pair + o, 128), width)
                terms.append(jnp.dot(b, wd[:, at], preferred_element_type=F32))
            term = jnp.concatenate(terms, 1)
            for t in range(2):
                for k in range(CORES):
                    for c in range(count):
                        row = c * CHUNK + half * k
                        send[2 * CORES * p + CORES * t + k, c] = term[row:row + half, t * cols:(t + 1) * cols].astype(BF16)
            for t in range(2 * CORES):
                to = 2 * CORES * p + t
                copy = piece(send.at[to], recv.at[me], ssem.at[to], rsem.at[me], to)
                if i:
                    copy.start()
                else:
                    pl.when(to != me)(copy.start)

    def gather2(first, count, send, recv, ssem, rsem, y, gsem, grsem):
        for i in order:
            frm = peer(i)
            piece(send.at[frm], recv.at[frm], ssem.at[frm], rsem.at[frm], frm).wait_recv()
        for c in range(count):
            total = send[me, c].astype(F32)
            for i in order:
                total += recv[peer(i), c].astype(F32)
            y[me, c] = (hg[first + c, me].astype(F32) + total).astype(BF16)
        for i in order:
            to = peer(i)
            piece(y.at[me], y.at[me], gsem.at[to], grsem.at[me], to).start()

    def collect2(first, count, y, gsem, grsem):
        for i in order:
            frm = peer(i)
            piece(y.at[frm], y.at[frm], gsem.at[frm], grsem.at[frm], frm).wait_recv()
        for c in range(count):
            for t in range(chips):
                both = jnp.concatenate([y[CORES * t + k, c].astype(F32) for k in range(CORES)], 0)
                out_ref[pl.ds((first + c) * CHUNK, CHUNK), pl.ds(t * cols, cols)] = both.astype(BF16)

    early = chunks - LATE
    mlp(0, early, send2, recv2, s2s.at[0], s2r.at[0])
    mlp(early, LATE, send3, recv3, s2s.at[1], s2r.at[1])
    gather2(0, early, send2, recv2, s2s.at[0], s2r.at[0], yg, g2s.at[0], g2r.at[0])
    gather2(early, LATE, send3, recv3, s2s.at[1], s2r.at[1], yh, g2s.at[1], g2r.at[1])
    collect2(0, early, yg, g2s.at[0], g2r.at[0])
    collect2(early, LATE, yh, g2s.at[1], g2r.at[1])

    for i in order:
        to = peer(i)
        for c in range(chunks):
            piece(hg.at[c, me], hg.at[c, me], g1s.at[c, to], g1r.at[c, me], to).wait_send()
        for at, send, y in ((0, send2, yg), (1, send3, yh)):
            piece(send.at[to], send.at[to], s2s.at[at, to], s2r.at[at, me], to).wait_send()
            piece(y.at[me], y.at[me], g2s.at[at, to], g2r.at[at, me], to).wait_send()
    for u in range(groups):
        for i in far:
            t = lax.rem(z + i, chips)
            copy = piece(send1.at[u, t], send1.at[u, t], s1s.at[u, t], s1r.at[u // CORES, me], me)
            if i:
                copy.wait_send()
            else:
                pl.when(core != u % CORES)(copy.wait_send)


def solution(mesh):
    n = mesh.shape["tp"]

    def step(x, k_cache, v_cache, gain_a, wq, wo, gain_m, w_gate, w_up, w_down):
        rows, d = x.shape
        cache = k_cache.shape[1]
        ff = w_gate.shape[1]
        k_cache, v_cache = k_cache.reshape(rows, cache, HEAD), v_cache.reshape(rows, cache, HEAD)
        chunks, half, cols = rows // CHUNK, CHUNK // CORES, d // (n // CORES)
        trig = jnp.asarray(rotary_table(cache, HEAD // 2))
        any_, vmem = pl.BlockSpec(memory_space=pl.ANY), pl.BlockSpec(memory_space=pltpu.VMEM)
        dma = pltpu.SemaphoreType.DMA
        return pl.pallas_call(
            functools.partial(layer, n),
            name="layer",
            out_shape=jax.ShapeDtypeStruct((rows, d), BF16),
            in_specs=[any_, any_, any_, vmem, vmem, any_, any_, vmem, any_, any_, any_],
            out_specs=vmem,
            scratch_shapes=[
                pltpu.VMEM((rows, d), BF16),
                pltpu.VMEM((rows, d), F32),
                pltpu.VMEM((rows, d), BF16),
                pltpu.VMEM(wq.shape, BF16),
                pltpu.VMEM(wo.shape, BF16),
                pltpu.VMEM(w_gate.shape, BF16),
                pltpu.VMEM(w_up.shape, BF16),
                pltpu.VMEM(w_down.shape, BF16),
                pltpu.VMEM((SLOTS, GROUP, cache, HEAD), BF16),
                pltpu.VMEM((SLOTS, GROUP, cache, HEAD), BF16),
                pltpu.VMEM((rows, HEAD), F32),
                pltpu.VMEM((rows, ff), BF16),
                pltpu.VMEM((rows // GROUP, n // CORES, half, cols), BF16),
                pltpu.VMEM((chunks, n, half, cols), BF16),
                pltpu.VMEM((chunks, n, half, cols), BF16),
                *[pltpu.VMEM((n, chunks - LATE, half, cols), BF16)] * 3,
                *[pltpu.VMEM((n, LATE, half, cols), BF16)] * 3,
                dma((6,)),
                dma((SLOTS,)),
                dma((SLOTS,)),
                dma((rows // GROUP, n // CORES)),
                dma((chunks, n)),
                dma((chunks, n)),
                dma((chunks, n)),
                dma((2, n)),
                dma((2, n)),
                dma((2, n)),
                dma((2, n)),
            ],
            compiler_params=pltpu.CompilerParams(
                collective_id=0, has_side_effects=True, vmem_limit_bytes=67_043_328
            ),
        )(x, k_cache, v_cache, gain_a.reshape(-1, 128), trig, wq, wo, gain_m.reshape(-1, 128), w_gate, w_up, w_down)

    states, cache, columns, rows_of = P("dp", None), P("dp", None, "tp", None), P(None, "tp"), P("tp", None)
    return jax.shard_map(
        step,
        mesh=mesh,
        in_specs=(states, cache, cache, P(None), columns, rows_of, P(None), columns, columns, rows_of),
        out_specs=states,
        check_vma=False,
    )
```

```python
import functools

import jax
import jax.numpy as jnp
import numpy as np
from jax import lax
from jax.experimental import pallas as pl
from jax.experimental.pallas import tpu as pltpu
from jax.sharding import PartitionSpec as P

HEAD = 256
THETA = 10000
CORES = 2
GROUP = 8
CHUNK = 16
SLOTS = 3
LATE = 1
UNROLL = True
MESH = pl.DeviceIdType.MESH
F32, BF16 = jnp.float32, jnp.bfloat16


def rotary_table(cache, half):
    angle = np.float32(cache - 1) * (np.float32(THETA) ** (-np.arange(half, dtype=np.float32) / half))
    return np.stack([np.cos(angle), np.sin(angle)]).astype(np.float32)


def layer(n, x_hbm, k_hbm, v_hbm, ga_ref, trig_ref, wq_hbm, wo_hbm, gm_ref, wg_hbm, wu_hbm, wd_hbm, out_ref,
          x16, xs, a16, wq, wo, wg, wu, wd, kbuf, vbuf, q32, hb,
          send1, recv1, hg, xs2, xr2, sz, rz, yg, send3, recv3, yh,
          in_sem, k_sem, v_sem, s1s, s1r, g1s, g1r, s2s, s2r, g2s, g2r, xss, xsr, zs, zr, ys, yr, fs, fr):
    rows, d = x16.shape
    ff = wg.shape[1]
    groups, chunks = rows // GROUP, rows // CHUNK
    half = CHUNK // CORES
    chips = n // CORES
    cols = d // chips
    me = lax.axis_index("tp")
    z, core = me // CORES, lax.rem(me, CORES)
    tiles = d // 128

    def peer(i):
        return lax.rem(me + i, n)

    order = sorted(range(1, n), key=lambda i: -min(i, n - i))
    far = [chips // 2]
    for i in range(chips // 2 - 1, 0, -1):
        far += [i, chips - i]
    far.append(0)

    load_x = pltpu.make_async_copy(x_hbm, x16, in_sem.at[0])
    load_wq = pltpu.make_async_copy(wq_hbm, wq, in_sem.at[1])
    load_wo = pltpu.make_async_copy(wo_hbm, wo, in_sem.at[2])
    load_wg = pltpu.make_async_copy(wg_hbm, wg, in_sem.at[3])
    load_wu = pltpu.make_async_copy(wu_hbm, wu, in_sem.at[4])
    load_wd = pltpu.make_async_copy(wd_hbm, wd, in_sem.at[5])

    def load_k(g):
        slot = lax.rem(g, SLOTS)
        return pltpu.make_async_copy(k_hbm.at[pl.ds(g * GROUP, GROUP)], kbuf.at[slot], k_sem.at[slot])

    def load_v(g):
        slot = lax.rem(g, SLOTS)
        return pltpu.make_async_copy(v_hbm.at[pl.ds(g * GROUP, GROUP)], vbuf.at[slot], v_sem.at[slot])

    load_x.start()
    load_wq.start()
    for g in range(SLOTS):
        load_k(g).start()
        load_v(g).start()
        if g == 0:
            load_wo.start()

    barrier = pltpu.get_barrier_semaphore()
    for i in range(1, n):
        pl.semaphore_signal(barrier, inc=1, device_id={"tp": peer(i)}, device_id_type=MESH)

    load_x.wait()
    part = jnp.zeros((rows, 128), F32)
    for j in range(tiles):
        block = x16[:, pl.ds(128 * j, 128)].astype(F32)
        xs[:, pl.ds(128 * j, 128)] = block
        part += block * block
    scale = lax.rsqrt(jnp.sum(part, -1, keepdims=True) / d + 1e-6)
    gain = ga_ref[...].astype(F32)
    for j in range(tiles):
        a16[:, pl.ds(128 * j, 128)] = (xs[:, pl.ds(128 * j, 128)] * scale * gain[j:j + 1]).astype(BF16)
    load_wq.wait()
    q = jnp.dot(a16[...], wq[...], preferred_element_type=F32).astype(BF16).astype(F32)
    turn = HEAD // 2
    cos, sin = trig_ref[0:1], trig_ref[1:2]
    qa, qb = q[:, :turn], q[:, turn:]
    q32[:, :turn] = (qa * cos - qb * sin).astype(BF16).astype(F32)
    q32[:, turn:] = (qb * cos + qa * sin).astype(BF16).astype(F32)

    pl.semaphore_wait(barrier, n - 1)

    def piece(src, dst, ssem, rsem, to):
        return pltpu.make_async_remote_copy(src_ref=src, dst_ref=dst, send_sem=ssem, recv_sem=rsem,
                                            device_id={"tp": to}, device_id_type=MESH)

    def term1(u, seen):
        term = jnp.concatenate([jnp.dot(seen, wo[:, pl.ds(o, 256)], preferred_element_type=F32) for o in range(0, d, 256)], 1)
        for t in range(chips):
            send1[u, t] = term[:, t * cols:(t + 1) * cols].astype(BF16)

    def scatter1(u):
        kind = lax.rem(u, CORES)
        c = u // CORES
        for i in far:
            t = lax.rem(z + i, chips)
            to = CORES * t + kind
            copy = piece(send1.at[u, t], recv1.at[c, me], s1s.at[u, t], s1r.at[c, me], to)
            if i:
                copy.start()
            else:
                pl.when(core != kind)(copy.start)

    def gather1(c):
        u = CORES * c + core
        total = send1[u, z].astype(F32)
        for i in order:
            frm = peer(i)
            piece(send1.at[u, z], recv1.at[c, frm], s1s.at[u, z], s1r.at[c, frm], frm).wait_recv()
        for i in order:
            total += recv1[c, peer(i)].astype(F32)
        at = pl.ds(pl.multiple_of(u * half, half), half)
        hg[c, me] = (xs[at, pl.ds(pl.multiple_of(z * cols, 128), cols)] + total).astype(BF16)
        for i in order:
            to = peer(i)
            piece(hg.at[c, me], hg.at[c, me], g1s.at[c, to], g1r.at[c, me], to).start()

    line = lax.broadcasted_iota(jnp.int32, (GROUP, 1), 0)

    def scores_of(g):
        slot = lax.rem(g, SLOTS)
        qg = q32[pl.ds(pl.multiple_of(g * GROUP, GROUP), GROUP), :]
        lhs = [jnp.where(line == i, qg, 0.0).astype(BF16) for i in range(GROUP)]
        out = []
        for j in range(kbuf.shape[2] // 256):
            total = None
            for i in range(GROUP):
                s = lax.dot_general(lhs[i], kbuf[slot, i, pl.ds(256 * j, 256)], (((1,), (1,)), ((), ())), preferred_element_type=F32)
                total = s if total is None else total + s
            out.append(total)
        return jnp.concatenate(out, 1) * HEAD**-0.5

    def seen_of(g, scores):
        slot = lax.rem(g, SLOTS)
        e = jnp.exp(scores - jnp.max(scores, -1, keepdims=True))
        w = e * (1.0 / jnp.sum(e, -1, keepdims=True))
        lhs = [jnp.where(line == i, w, 0.0).astype(BF16) for i in range(GROUP)]
        out = []
        for j in range(HEAD // 128):
            total = None
            for i in range(GROUP):
                s = jnp.dot(lhs[i], vbuf[slot, i, :, pl.ds(128 * j, 128)], preferred_element_type=F32)
                total = s if total is None else total + s
            out.append(total)
        return jnp.concatenate(out, 1).astype(BF16)

    def attend(g, scores):
        load_v(g).wait()
        load_k(g + 1).wait()
        later = scores_of(g + 1)
        seen = seen_of(g, scores)
        term1(g, seen)

        @pl.when(g + SLOTS < groups)
        def _():
            load_v(g + SLOTS).start()

        @pl.when(g + 1 + SLOTS < groups)
        def _():
            load_k(g + 1 + SLOTS).start()

        @pl.when(g == groups - SLOTS - 1)
        def _():
            load_wg.start()
            load_wu.start()
            load_wd.start()

        scatter1(g)

        @pl.when((lax.rem(g, CORES) == 0) & (g >= 2 * CORES))
        def _():
            gather1(g // CORES - 2)

        return later

    load_k(0).wait()
    scores = scores_of(0)
    load_k(SLOTS).start()
    load_wo.wait()
    scores = lax.fori_loop(0, groups - 1, attend, scores)
    load_v(groups - 1).wait()
    term1(groups - 1, seen_of(groups - 1, scores))
    scatter1(groups - 1)
    for c in range(chunks - 2, chunks):
        gather1(c)

    gain_m = gm_ref[...].astype(F32)
    width = 256
    pair = 2 * cols
    pairs = chips // 2

    early = chunks - LATE
    far_pairs = ((pairs // 2, 1), (pairs - 1, 0)) if pairs > 2 else ((1,), (0,))
    partner = CORES * z + 1 - core

    def mlp(first, count, send):
        for c in range(first, first + count):
            for i in order:
                frm = peer(i)
                piece(hg.at[c, frm], hg.at[c, frm], g1s.at[c, frm], g1r.at[c, frm], frm).wait_recv()
            blocks = []
            part = jnp.zeros((CHUNK, 128), F32)
            for t in range(chips):
                block = jnp.concatenate([hg[c, CORES * t + k].astype(F32) for k in range(CORES)], 0)
                for u in range(cols // 128):
                    sub = block[:, 128 * u:128 * (u + 1)]
                    blocks.append(sub)
                    part += sub * sub
            scale = lax.rsqrt(jnp.sum(part, -1, keepdims=True) / d + 1e-6)
            for j in range(tiles):
                a16[pl.ds(c * CHUNK, CHUNK), pl.ds(128 * j, 128)] = (blocks[j] * scale * gain_m[j:j + 1]).astype(BF16)

        mine = pl.ds(first * CHUNK, count * CHUNK)
        if first == 0:
            load_wg.wait()
            load_wu.wait()

        def hidden(j, _):
            at = pl.ds(pl.multiple_of(j * width, width), width)
            b = a16[mine, :]
            gate = jnp.dot(b, wg[:, at], preferred_element_type=F32)
            up = jnp.dot(b, wu[:, at], preferred_element_type=F32)
            hb[mine, at] = (gate / (1.0 + jnp.exp(-gate)) * up).astype(BF16)
            return 0

        lax.fori_loop(0, ff // width, hidden, 0, unroll=UNROLL)
        if first == 0:
            load_wd.wait()

        b = hb[mine, :]
        for h in range(2):
            blocks = [(lax.rem(z // 2 + i, pairs), i) for i in far_pairs[h]]
            terms = [[jnp.dot(b, wd[:, pl.ds(pl.multiple_of(p * pair + o, 128), width)], preferred_element_type=F32)
                      for o in range(0, pair, width)] for p, i in blocks]
            send(h, blocks, [jnp.concatenate(t, 1).astype(BF16) for t in terms])

    def unit(term, c, k, t):
        row = c * CHUNK + half * k
        return term[row:row + half, t * cols:(t + 1) * cols]

    def scatter_late(h, blocks, terms):
        for (p, i), term in zip(blocks, terms):
            for t in range(2):
                for k in range(CORES):
                    for c in range(LATE):
                        send3[2 * CORES * p + CORES * t + k, c] = unit(term, c, k, t)
        for p, i in blocks:
            for t in range(2 * CORES):
                to = 2 * CORES * p + t
                copy = piece(send3.at[to], recv3.at[me], s2s.at[to], s2r.at[me], to)
                if i:
                    copy.start()
                else:
                    pl.when(to != me)(copy.start)

    def swap(h):
        return piece(xs2.at[h, 1 - core], xr2.at[h], xss.at[h], xsr.at[h], partner)

    def scatter_early(h, blocks, terms):
        for b, term in enumerate(terms):
            for t in range(2):
                for k in range(CORES):
                    for c in range(early):
                        xs2[h, k, 2 * b + t, c] = unit(term, c, k, t)
        swap(h).start()

    def chip_piece(h, j, t):
        return piece(sz.at[h, j], rz.at[z], zs.at[h, j], zr.at[z], CORES * t + core)

    def scatter_chips(h):
        swap(h).wait_recv()
        for b, i in enumerate(far_pairs[h]):
            for t in range(2):
                j = 2 * b + t
                sz[h, j] = (xs2[h, core, j].astype(F32) + xr2[h, j].astype(F32)).astype(BF16)
        for b, i in enumerate(far_pairs[h]):
            for t in range(2):
                to = 2 * lax.rem(z // 2 + i, pairs) + t
                copy = chip_piece(h, 2 * b + t, to)
                if i:
                    copy.start()
                else:
                    pl.when(to != z)(copy.start)

    def y_piece(t, to):
        return piece(yg.at[core, t], yg.at[core, t], ys.at[to], yr.at[t], CORES * to + core)

    def gather_early():
        for i in far[:-1]:
            t = lax.rem(z + i, chips)
            piece(rz.at[t], rz.at[t], zs.at[0, 0], zr.at[t], me).wait_recv()
        total = sz[1, 2 + lax.rem(z, 2)].astype(F32)
        for i in far[:-1]:
            total += rz[lax.rem(z + i, chips)].astype(F32)
        for c in range(early):
            yg[core, z, c] = (hg[c, me].astype(F32) + total[c]).astype(BF16)
        for i in far[:-1]:
            y_piece(z, lax.rem(z + i, chips)).start()

    def forward():
        return piece(yg.at[core], yg.at[core], fs.at[0], fr.at[0], partner)

    def forward_early():
        for i in far[:-1]:
            t = lax.rem(z + i, chips)
            y_piece(t, t).wait_recv()
        forward().start()

    def collect_early():
        forward().wait_recv()
        for c in range(early):
            for t in range(chips):
                both = jnp.concatenate([yg[k, t, c].astype(F32) for k in range(CORES)], 0)
                out_ref[pl.ds(c * CHUNK, CHUNK), pl.ds(t * cols, cols)] = both.astype(BF16)

    def gather2(first, count, send, recv, ssem, rsem, y, gsem, grsem):
        for i in order:
            frm = peer(i)
            piece(send.at[frm], recv.at[frm], ssem.at[frm], rsem.at[frm], frm).wait_recv()
        for c in range(count):
            total = send[me, c].astype(F32)
            for i in order:
                total += recv[peer(i), c].astype(F32)
            y[me, c] = (hg[first + c, me].astype(F32) + total).astype(BF16)
        for i in order:
            to = peer(i)
            piece(y.at[me], y.at[me], gsem.at[to], grsem.at[me], to).start()

    def collect2(first, count, y, gsem, grsem):
        for i in order:
            frm = peer(i)
            piece(y.at[frm], y.at[frm], gsem.at[frm], grsem.at[frm], frm).wait_recv()
        for c in range(count):
            for t in range(chips):
                both = jnp.concatenate([y[CORES * t + k, c].astype(F32) for k in range(CORES)], 0)
                out_ref[pl.ds((first + c) * CHUNK, CHUNK), pl.ds(t * cols, cols)] = both.astype(BF16)

    mlp(0, early, scatter_early)
    scatter_chips(0)
    scatter_chips(1)
    mlp(early, LATE, scatter_late)
    gather_early()
    gather2(early, LATE, send3, recv3, s2s, s2r, yh, g2s, g2r)
    forward_early()
    collect_early()
    collect2(early, LATE, yh, g2s, g2r)

    for i in order:
        to = peer(i)
        for c in range(chunks):
            piece(hg.at[c, me], hg.at[c, me], g1s.at[c, to], g1r.at[c, me], to).wait_send()
        piece(send3.at[to], send3.at[to], s2s.at[to], s2r.at[me], to).wait_send()
        piece(yh.at[me], yh.at[me], g2s.at[to], g2r.at[me], to).wait_send()
    for h in range(2):
        swap(h).wait_send()
        for b, i in enumerate(far_pairs[h]):
            for t in range(2):
                to = 2 * lax.rem(z // 2 + i, pairs) + t
                copy = chip_piece(h, 2 * b + t, to)
                if i:
                    copy.wait_send()
                else:
                    pl.when(to != z)(copy.wait_send)
    for i in far[:-1]:
        y_piece(z, lax.rem(z + i, chips)).wait_send()
    forward().wait_send()
    for u in range(groups):
        for i in far:
            t = lax.rem(z + i, chips)
            copy = piece(send1.at[u, t], send1.at[u, t], s1s.at[u, t], s1r.at[u // CORES, me], me)
            if i:
                copy.wait_send()
            else:
                pl.when(core != u % CORES)(copy.wait_send)


def solution(mesh):
    n = mesh.shape["tp"]

    def step(x, k_cache, v_cache, gain_a, wq, wo, gain_m, w_gate, w_up, w_down):
        rows, d = x.shape
        cache = k_cache.shape[1]
        ff = w_gate.shape[1]
        k_cache, v_cache = k_cache.reshape(rows, cache, HEAD), v_cache.reshape(rows, cache, HEAD)
        chunks, half, cols = rows // CHUNK, CHUNK // CORES, d // (n // CORES)
        early = (chunks - LATE, half, cols)
        trig = jnp.asarray(rotary_table(cache, HEAD // 2))
        any_, vmem = pl.BlockSpec(memory_space=pl.ANY), pl.BlockSpec(memory_space=pltpu.VMEM)
        dma = pltpu.SemaphoreType.DMA
        return pl.pallas_call(
            functools.partial(layer, n),
            name="layer",
            out_shape=jax.ShapeDtypeStruct((rows, d), BF16),
            in_specs=[any_, any_, any_, vmem, vmem, any_, any_, vmem, any_, any_, any_],
            out_specs=vmem,
            scratch_shapes=[
                pltpu.VMEM((rows, d), BF16),
                pltpu.VMEM((rows, d), F32),
                pltpu.VMEM((rows, d), BF16),
                pltpu.VMEM(wq.shape, BF16),
                pltpu.VMEM(wo.shape, BF16),
                pltpu.VMEM(w_gate.shape, BF16),
                pltpu.VMEM(w_up.shape, BF16),
                pltpu.VMEM(w_down.shape, BF16),
                pltpu.VMEM((SLOTS, GROUP, cache, HEAD), BF16),
                pltpu.VMEM((SLOTS, GROUP, cache, HEAD), BF16),
                pltpu.VMEM((rows, HEAD), F32),
                pltpu.VMEM((rows, ff), BF16),
                pltpu.VMEM((rows // GROUP, n // CORES, half, cols), BF16),
                pltpu.VMEM((chunks, n, half, cols), BF16),
                pltpu.VMEM((chunks, n, half, cols), BF16),
                pltpu.VMEM((2, CORES, n // CORES // 2, *early), BF16),
                pltpu.VMEM((2, n // CORES // 2, *early), BF16),
                pltpu.VMEM((2, n // CORES // 2, *early), BF16),
                pltpu.VMEM((n // CORES, *early), BF16),
                pltpu.VMEM((CORES, n // CORES, *early), BF16),
                *[pltpu.VMEM((n, LATE, half, cols), BF16)] * 3,
                dma((6,)),
                dma((SLOTS,)),
                dma((SLOTS,)),
                dma((rows // GROUP, n // CORES)),
                dma((chunks, n)),
                dma((chunks, n)),
                dma((chunks, n)),
                *[dma((n,))] * 4,
                *[dma((2,))] * 2,
                dma((2, n // CORES // 2)),
                *[dma((n // CORES,))] * 3,
                *[dma((1,))] * 2,
            ],
            compiler_params=pltpu.CompilerParams(
                collective_id=0, has_side_effects=True, vmem_limit_bytes=67_043_328
            ),
        )(x, k_cache, v_cache, gain_a.reshape(-1, 128), trig, wq, wo, gain_m.reshape(-1, 128), w_gate, w_up, w_down)

    states, cache, columns, rows_of = P("dp", None), P("dp", None, "tp", None), P(None, "tp"), P("tp", None)
    return jax.shard_map(
        step,
        mesh=mesh,
        in_specs=(states, cache, cache, P(None), columns, rows_of, P(None), columns, columns, rows_of),
        out_specs=states,
        check_vma=False,
    )
```

```python
import functools

import jax
import jax.numpy as jnp
import numpy as np
from jax import lax
from jax.experimental import pallas as pl
from jax.experimental.pallas import tpu as pltpu
from jax.sharding import PartitionSpec as P

HEAD = 256
THETA = 10000
CORES = 2
GROUP = 8
CHUNK = 16
SLOTS = 3
STAGES = 2
MESH = pl.DeviceIdType.MESH
F32, BF16 = jnp.float32, jnp.bfloat16


def rotary_table(cache, half):
    angle = np.float32(cache - 1) * (np.float32(THETA) ** (-np.arange(half, dtype=np.float32) / half))
    return np.stack([np.cos(angle), np.sin(angle)]).astype(np.float32)


def layer(n, x_hbm, k_hbm, v_hbm, ga_ref, trig_ref, wq_hbm, wo_hbm, gm_ref, wg_hbm, wu_hbm, wd_hbm, out_ref,
          x16, xs, a16, wq, wo, wg, wu, wd, kbuf, vbuf, q32, hb,
          send1, recv1, hg, xs2, xr2, sz, rz, yg,
          in_sem, k_sem, v_sem, s1s, s1r, g1s, g1r, xss, xsr, zs, zr, ys, yr, fs, fr):
    rows, d = x16.shape
    ff = wg.shape[1]
    groups, chunks = rows // GROUP, rows // CHUNK
    half = CHUNK // CORES
    chips = n // CORES
    cols = d // chips
    me = lax.axis_index("tp")
    z, core = me // CORES, lax.rem(me, CORES)
    tiles = d // 128

    def peer(i):
        return lax.rem(me + i, n)

    order = sorted(range(1, n), key=lambda i: -min(i, n - i))
    far = [chips // 2]
    for i in range(chips // 2 - 1, 0, -1):
        far += [i, chips - i]
    far.append(0)

    load_x = pltpu.make_async_copy(x_hbm, x16, in_sem.at[0])
    load_wq = pltpu.make_async_copy(wq_hbm, wq, in_sem.at[1])
    load_wo = pltpu.make_async_copy(wo_hbm, wo, in_sem.at[2])
    load_wg = pltpu.make_async_copy(wg_hbm, wg, in_sem.at[3])
    load_wu = pltpu.make_async_copy(wu_hbm, wu, in_sem.at[4])
    load_wd = pltpu.make_async_copy(wd_hbm, wd, in_sem.at[5])

    def load_k(g):
        slot = lax.rem(g, SLOTS)
        return pltpu.make_async_copy(k_hbm.at[pl.ds(g * GROUP, GROUP)], kbuf.at[slot], k_sem.at[slot])

    def load_v(g):
        slot = lax.rem(g, SLOTS)
        return pltpu.make_async_copy(v_hbm.at[pl.ds(g * GROUP, GROUP)], vbuf.at[slot], v_sem.at[slot])

    load_x.start()
    load_wq.start()
    for g in range(SLOTS):
        load_k(g).start()
        load_v(g).start()
        if g == 0:
            load_wo.start()

    barrier = pltpu.get_barrier_semaphore()
    for i in range(1, n):
        pl.semaphore_signal(barrier, inc=1, device_id={"tp": peer(i)}, device_id_type=MESH)

    load_x.wait()
    part = jnp.zeros((rows, 128), F32)
    for j in range(tiles):
        block = x16[:, pl.ds(128 * j, 128)].astype(F32)
        xs[:, pl.ds(128 * j, 128)] = block
        part += block * block
    scale = lax.rsqrt(jnp.sum(part, -1, keepdims=True) / d + 1e-6)
    gain = ga_ref[...].astype(F32)
    for j in range(tiles):
        a16[:, pl.ds(128 * j, 128)] = (xs[:, pl.ds(128 * j, 128)] * scale * gain[j:j + 1]).astype(BF16)
    load_wq.wait()
    q = jnp.dot(a16[...], wq[...], preferred_element_type=F32).astype(BF16).astype(F32)
    turn = HEAD // 2
    cos, sin = trig_ref[0:1], trig_ref[1:2]
    qa, qb = q[:, :turn], q[:, turn:]
    q32[:, :turn] = (qa * cos - qb * sin).astype(BF16).astype(F32)
    q32[:, turn:] = (qb * cos + qa * sin).astype(BF16).astype(F32)

    pl.semaphore_wait(barrier, n - 1)

    def piece(src, dst, ssem, rsem, to):
        return pltpu.make_async_remote_copy(src_ref=src, dst_ref=dst, send_sem=ssem, recv_sem=rsem,
                                            device_id={"tp": to}, device_id_type=MESH)

    def term1(u, seen):
        term = jnp.concatenate([jnp.dot(seen, wo[:, pl.ds(o, 256)], preferred_element_type=F32) for o in range(0, d, 256)], 1)
        for t in range(chips):
            send1[u, t] = term[:, t * cols:(t + 1) * cols].astype(BF16)

    def scatter1(u):
        kind = lax.rem(u, CORES)
        c = u // CORES
        for i in far:
            t = lax.rem(z + i, chips)
            to = CORES * t + kind
            copy = piece(send1.at[u, t], recv1.at[c, me], s1s.at[u, t], s1r.at[c, me], to)
            if i:
                copy.start()
            else:
                pl.when(core != kind)(copy.start)

    def gather1(c):
        u = CORES * c + core
        total = send1[u, z].astype(F32)
        for i in order:
            frm = peer(i)
            piece(send1.at[u, z], recv1.at[c, frm], s1s.at[u, z], s1r.at[c, frm], frm).wait_recv()
        for i in order:
            total += recv1[c, peer(i)].astype(F32)
        at = pl.ds(pl.multiple_of(u * half, half), half)
        hg[c, me] = (xs[at, pl.ds(pl.multiple_of(z * cols, 128), cols)] + total).astype(BF16)
        for i in order:
            to = peer(i)
            piece(hg.at[c, me], hg.at[c, me], g1s.at[c, to], g1r.at[c, me], to).start()

    line = lax.broadcasted_iota(jnp.int32, (GROUP, 1), 0)

    def scores_of(g):
        slot = lax.rem(g, SLOTS)
        qg = q32[pl.ds(pl.multiple_of(g * GROUP, GROUP), GROUP), :]
        lhs = [jnp.where(line == i, qg, 0.0).astype(BF16) for i in range(GROUP)]
        out = []
        for j in range(kbuf.shape[2] // 256):
            total = None
            for i in range(GROUP):
                s = lax.dot_general(lhs[i], kbuf[slot, i, pl.ds(256 * j, 256)], (((1,), (1,)), ((), ())), preferred_element_type=F32)
                total = s if total is None else total + s
            out.append(total)
        return jnp.concatenate(out, 1) * HEAD**-0.5

    def seen_of(g, scores):
        slot = lax.rem(g, SLOTS)
        e = jnp.exp(scores - jnp.max(scores, -1, keepdims=True))
        w = e * (1.0 / jnp.sum(e, -1, keepdims=True))
        lhs = [jnp.where(line == i, w, 0.0).astype(BF16) for i in range(GROUP)]
        out = []
        for j in range(HEAD // 128):
            total = None
            for i in range(GROUP):
                s = jnp.dot(lhs[i], vbuf[slot, i, :, pl.ds(128 * j, 128)], preferred_element_type=F32)
                total = s if total is None else total + s
            out.append(total)
        return jnp.concatenate(out, 1).astype(BF16)

    def attend(g, scores):
        load_v(g).wait()
        load_k(g + 1).wait()
        later = scores_of(g + 1)
        seen = seen_of(g, scores)
        term1(g, seen)

        @pl.when(g + SLOTS < groups)
        def _():
            load_v(g + SLOTS).start()

        @pl.when(g + 1 + SLOTS < groups)
        def _():
            load_k(g + 1 + SLOTS).start()

        @pl.when(g == groups - SLOTS - 1)
        def _():
            load_wg.start()
            load_wu.start()
            load_wd.start()

        scatter1(g)

        @pl.when((lax.rem(g, CORES) == 0) & (g >= 2 * CORES))
        def _():
            gather1(g // CORES - 2)

        return later

    load_k(0).wait()
    scores = scores_of(0)
    load_k(SLOTS).start()
    load_wo.wait()
    scores = lax.fori_loop(0, groups - 1, attend, scores)
    load_v(groups - 1).wait()
    term1(groups - 1, seen_of(groups - 1, scores))
    scatter1(groups - 1)
    for c in range(chunks - 2, chunks):
        gather1(c)

    gain_m = gm_ref[...].astype(F32)
    width = 256

    partner = CORES * z + 1 - core
    others = far[:-1]
    deep = chunks // STAGES

    for c in range(chunks):
        for i in order:
            frm = peer(i)
            piece(hg.at[c, frm], hg.at[c, frm], g1s.at[c, frm], g1r.at[c, frm], frm).wait_recv()
        blocks = []
        part = jnp.zeros((CHUNK, 128), F32)
        for t in range(chips):
            block = jnp.concatenate([hg[c, CORES * t + k].astype(F32) for k in range(CORES)], 0)
            for u in range(cols // 128):
                sub = block[:, 128 * u:128 * (u + 1)]
                blocks.append(sub)
                part += sub * sub
        scale = lax.rsqrt(jnp.sum(part, -1, keepdims=True) / d + 1e-6)
        for j in range(tiles):
            a16[pl.ds(c * CHUNK, CHUNK), pl.ds(128 * j, 128)] = (blocks[j] * scale * gain_m[j:j + 1]).astype(BF16)

    load_wg.wait()
    load_wu.wait()
    for j in range(ff // width):
        at = pl.ds(j * width, width)
        b = a16[...]
        gate = jnp.dot(b, wg[:, at], preferred_element_type=F32)
        up = jnp.dot(b, wu[:, at], preferred_element_type=F32)
        hb[:, at] = (gate / (1.0 + jnp.exp(-gate)) * up).astype(BF16)
    load_wd.wait()

    def swap(s):
        return piece(xs2.at[s, 1 - core], xr2.at[s], xss.at[s], xsr.at[s], partner)

    def chip_piece(s, t):
        return piece(sz.at[s, t], rz.at[s, z], zs.at[s, t], zr.at[s, z], CORES * t + core)

    def y_piece(s, t, to):
        return piece(yg.at[s, core, t], yg.at[s, core, t], ys.at[s, to], yr.at[s, t], CORES * to + core)

    def forward(s):
        return piece(yg.at[s, core], yg.at[s, core], fs.at[s], fr.at[s], partner)

    b = hb[...]
    term = jnp.concatenate([jnp.dot(b, wd[:, pl.ds(o, width)], preferred_element_type=F32).astype(BF16)
                            for o in range(0, d, width)], 1)
    for s in range(STAGES):
        for k in range(CORES):
            for t in range(chips):
                for c in range(deep):
                    row = (s * deep + c) * CHUNK + half * k
                    xs2[s, k, t, c] = term[row:row + half, t * cols:(t + 1) * cols]
        swap(s).start()
    for s in range(STAGES):
        swap(s).wait_recv()
        for t in range(chips):
            sz[s, t] = (xs2[s, core, t].astype(F32) + xr2[s, t].astype(F32)).astype(BF16)
        for i in others:
            chip_piece(s, lax.rem(z + i, chips)).start()
    for s in range(STAGES):
        for i in others:
            t = lax.rem(z + i, chips)
            piece(rz.at[s, t], rz.at[s, t], zs.at[s, t], zr.at[s, t], me).wait_recv()
        total = sz[s, z].astype(F32)
        for i in others:
            total += rz[s, lax.rem(z + i, chips)].astype(F32)
        for c in range(deep):
            yg[s, core, z, c] = (hg[s * deep + c, me].astype(F32) + total[c]).astype(BF16)
        for i in others:
            y_piece(s, z, lax.rem(z + i, chips)).start()
    for s in range(STAGES):
        for i in others:
            t = lax.rem(z + i, chips)
            y_piece(s, t, t).wait_recv()
        forward(s).start()
    for s in range(STAGES):
        forward(s).wait_recv()
        for c in range(deep):
            for t in range(chips):
                both = jnp.concatenate([yg[s, k, t, c].astype(F32) for k in range(CORES)], 0)
                out_ref[pl.ds((s * deep + c) * CHUNK, CHUNK), pl.ds(t * cols, cols)] = both.astype(BF16)

    for i in order:
        to = peer(i)
        for c in range(chunks):
            piece(hg.at[c, me], hg.at[c, me], g1s.at[c, to], g1r.at[c, me], to).wait_send()
    for s in range(STAGES):
        swap(s).wait_send()
        forward(s).wait_send()
        for i in others:
            t = lax.rem(z + i, chips)
            chip_piece(s, t).wait_send()
            y_piece(s, z, t).wait_send()
    for u in range(groups):
        for i in far:
            t = lax.rem(z + i, chips)
            copy = piece(send1.at[u, t], send1.at[u, t], s1s.at[u, t], s1r.at[u // CORES, me], me)
            if i:
                copy.wait_send()
            else:
                pl.when(core != u % CORES)(copy.wait_send)


def solution(mesh):
    n = mesh.shape["tp"]

    def step(x, k_cache, v_cache, gain_a, wq, wo, gain_m, w_gate, w_up, w_down):
        rows, d = x.shape
        cache = k_cache.shape[1]
        ff = w_gate.shape[1]
        k_cache, v_cache = k_cache.reshape(rows, cache, HEAD), v_cache.reshape(rows, cache, HEAD)
        chunks, half, cols = rows // CHUNK, CHUNK // CORES, d // (n // CORES)
        deep = (chunks // STAGES, half, cols)
        trig = jnp.asarray(rotary_table(cache, HEAD // 2))
        any_, vmem = pl.BlockSpec(memory_space=pl.ANY), pl.BlockSpec(memory_space=pltpu.VMEM)
        dma = pltpu.SemaphoreType.DMA
        return pl.pallas_call(
            functools.partial(layer, n),
            name="layer",
            out_shape=pltpu.VMEM((rows, d), BF16),
            in_specs=[any_, any_, any_, vmem, vmem, any_, any_, vmem, any_, any_, any_],
            out_specs=vmem,
            scratch_shapes=[
                pltpu.VMEM((rows, d), BF16),
                pltpu.VMEM((rows, d), F32),
                pltpu.VMEM((rows, d), BF16),
                pltpu.VMEM(wq.shape, BF16),
                pltpu.VMEM(wo.shape, BF16),
                pltpu.VMEM(w_gate.shape, BF16),
                pltpu.VMEM(w_up.shape, BF16),
                pltpu.VMEM(w_down.shape, BF16),
                pltpu.VMEM((SLOTS, GROUP, cache, HEAD), BF16),
                pltpu.VMEM((SLOTS, GROUP, cache, HEAD), BF16),
                pltpu.VMEM((rows, HEAD), F32),
                pltpu.VMEM((rows, ff), BF16),
                pltpu.VMEM((rows // GROUP, n // CORES, half, cols), BF16),
                pltpu.VMEM((chunks, n, half, cols), BF16),
                pltpu.VMEM((chunks, n, half, cols), BF16),
                pltpu.VMEM((STAGES, CORES, n // CORES, *deep), BF16),
                *[pltpu.VMEM((STAGES, n // CORES, *deep), BF16)] * 3,
                pltpu.VMEM((STAGES, CORES, n // CORES, *deep), BF16),
                dma((6,)),
                dma((SLOTS,)),
                dma((SLOTS,)),
                dma((rows // GROUP, n // CORES)),
                dma((chunks, n)),
                dma((chunks, n)),
                dma((chunks, n)),
                *[dma((STAGES,))] * 2,
                *[dma((STAGES, n // CORES))] * 4,
                *[dma((STAGES,))] * 2,
            ],
            compiler_params=pltpu.CompilerParams(
                collective_id=0, has_side_effects=True, vmem_limit_bytes=60 * 1024 * 1024
            ),
        )(x, k_cache, v_cache, gain_a.reshape(-1, 128), trig, wq, wo, gain_m.reshape(-1, 128), w_gate, w_up, w_down)

    states, cache, columns, rows_of = P("dp", None), P("dp", None, "tp", None), P(None, "tp"), P("tp", None)
    return jax.shard_map(
        step,
        mesh=mesh,
        in_specs=(states, cache, cache, P(None), columns, rows_of, P(None), columns, columns, rows_of),
        out_specs=states,
        check_vma=False,
    )
```

```python
import functools

import jax
import jax.numpy as jnp
import numpy as np
from jax import lax
from jax.experimental import pallas as pl
from jax.experimental.pallas import tpu as pltpu
from jax.sharding import PartitionSpec as P

HEAD = 256
THETA = 10000
CORES = 2
GROUP = 8
CHUNK = 16
SLOTS = 3
LATE = 1
UNROLL = True
MESH = pl.DeviceIdType.MESH
F32, BF16 = jnp.float32, jnp.bfloat16


def rotary_table(cache, half):
    angle = np.float32(cache - 1) * (np.float32(THETA) ** (-np.arange(half, dtype=np.float32) / half))
    return np.stack([np.cos(angle), np.sin(angle)]).astype(np.float32)


def layer(n, x_hbm, k_hbm, v_hbm, ga_ref, trig_ref, wq_hbm, wo_hbm, gm_ref, wg_hbm, wu_hbm, wd_hbm, out_ref,
          x16, xs, a16, wq, wo, wg, wu, wd, kbuf, vbuf, q32, hb,
          send1, recv1, hg, xs2, xr2, sz, rz, yg, send3, recv3, yh,
          in_sem, k_sem, v_sem, s1s, s1r, g1s, g1r, s2s, s2r, g2s, g2r, xss, xsr, zs, zr, ys, yr, fs, fr):
    rows, d = x16.shape
    ff = wg.shape[1]
    groups, chunks = rows // GROUP, rows // CHUNK
    half = CHUNK // CORES
    chips = n // CORES
    cols = d // chips
    me = lax.axis_index("tp")
    z, core = me // CORES, lax.rem(me, CORES)
    tiles = d // 128

    def peer(i):
        return lax.rem(me + i, n)

    order = sorted(range(1, n), key=lambda i: -min(i, n - i))
    far = [chips // 2]
    for i in range(chips // 2 - 1, 0, -1):
        far += [i, chips - i]
    far.append(0)

    load_x = pltpu.make_async_copy(x_hbm, x16, in_sem.at[0])
    load_wq = pltpu.make_async_copy(wq_hbm, wq, in_sem.at[1])
    load_wo = pltpu.make_async_copy(wo_hbm, wo, in_sem.at[2])
    load_wg = pltpu.make_async_copy(wg_hbm, wg, in_sem.at[3])
    load_wu = pltpu.make_async_copy(wu_hbm, wu, in_sem.at[4])
    load_wd = pltpu.make_async_copy(wd_hbm, wd, in_sem.at[5])

    def load_k(g):
        slot = lax.rem(g, SLOTS)
        return pltpu.make_async_copy(k_hbm.at[pl.ds(g * GROUP, GROUP)], kbuf.at[slot], k_sem.at[slot])

    def load_v(g):
        slot = lax.rem(g, SLOTS)
        return pltpu.make_async_copy(v_hbm.at[pl.ds(g * GROUP, GROUP)], vbuf.at[slot], v_sem.at[slot])

    load_x.start()
    load_wq.start()
    for g in range(SLOTS):
        load_k(g).start()
        load_v(g).start()
        if g == 0:
            load_wo.start()

    barrier = pltpu.get_barrier_semaphore()
    for i in range(1, n):
        pl.semaphore_signal(barrier, inc=1, device_id={"tp": peer(i)}, device_id_type=MESH)

    load_x.wait()
    part = jnp.zeros((rows, 128), F32)
    for j in range(tiles):
        block = x16[:, pl.ds(128 * j, 128)].astype(F32)
        xs[:, pl.ds(128 * j, 128)] = block
        part += block * block
    scale = lax.rsqrt(jnp.sum(part, -1, keepdims=True) / d + 1e-6)
    gain = ga_ref[...].astype(F32)
    for j in range(tiles):
        a16[:, pl.ds(128 * j, 128)] = (xs[:, pl.ds(128 * j, 128)] * scale * gain[j:j + 1]).astype(BF16)
    load_wq.wait()
    q = [jnp.dot(a16[...], wq[:, pl.ds(o, 128)], preferred_element_type=F32).astype(BF16).astype(F32) for o in range(0, HEAD, 128)]
    q = jnp.concatenate(q, 1)
    turn = HEAD // 2
    cos, sin = trig_ref[0:1], trig_ref[1:2]
    qa, qb = q[:, :turn], q[:, turn:]
    q32[:, :turn] = (qa * cos - qb * sin).astype(BF16).astype(F32)
    q32[:, turn:] = (qb * cos + qa * sin).astype(BF16).astype(F32)

    def piece(src, dst, ssem, rsem, to):
        return pltpu.make_async_remote_copy(src_ref=src, dst_ref=dst, send_sem=ssem, recv_sem=rsem,
                                            device_id={"tp": to}, device_id_type=MESH)

    def term1(u, seen):
        term = jnp.concatenate([jnp.dot(seen, wo[:, pl.ds(o, 256)], preferred_element_type=F32) for o in range(0, d, 256)], 1)
        for t in range(chips):
            send1[u, t] = term[:, t * cols:(t + 1) * cols].astype(BF16)

    def scatter1(u):
        kind = lax.rem(u, CORES)
        c = u // CORES
        for i in far:
            t = lax.rem(z + i, chips)
            to = CORES * t + kind
            copy = piece(send1.at[u, t], recv1.at[c, me], s1s.at[u, t], s1r.at[c, me], to)
            if i:
                copy.start()
            else:
                pl.when(core != kind)(copy.start)

    def gather1(c):
        u = CORES * c + core
        total = send1[u, z].astype(F32)
        for i in order:
            frm = peer(i)
            piece(send1.at[u, z], recv1.at[c, frm], s1s.at[u, z], s1r.at[c, frm], frm).wait_recv()
        for i in order:
            total += recv1[c, peer(i)].astype(F32)
        at = pl.ds(pl.multiple_of(u * half, half), half)
        hg[c, me] = (xs[at, pl.ds(pl.multiple_of(z * cols, 128), cols)] + total).astype(BF16)
        for i in order:
            to = peer(i)
            piece(hg.at[c, me], hg.at[c, me], g1s.at[c, to], g1r.at[c, me], to).start()

    line = lax.broadcasted_iota(jnp.int32, (GROUP, 1), 0)

    def scores_of(g):
        slot = lax.rem(g, SLOTS)
        qg = q32[pl.ds(pl.multiple_of(g * GROUP, GROUP), GROUP), :]
        lhs = [jnp.where(line == i, qg, 0.0).astype(BF16) for i in range(GROUP)]
        out = []
        for j in range(kbuf.shape[2] // 256):
            total = None
            for i in range(GROUP):
                s = lax.dot_general(lhs[i], kbuf[slot, i, pl.ds(256 * j, 256)], (((1,), (1,)), ((), ())), preferred_element_type=F32)
                total = s if total is None else total + s
            out.append(total)
        return jnp.concatenate(out, 1) * HEAD**-0.5

    def seen_of(g, scores):
        slot = lax.rem(g, SLOTS)
        e = jnp.exp(scores - jnp.max(scores, -1, keepdims=True))
        w = e * (1.0 / jnp.sum(e, -1, keepdims=True))
        lhs = [jnp.where(line == i, w, 0.0).astype(BF16) for i in range(GROUP)]
        out = []
        for j in range(HEAD // 128):
            total = None
            for i in range(GROUP):
                s = jnp.dot(lhs[i], vbuf[slot, i, :, pl.ds(128 * j, 128)], preferred_element_type=F32)
                total = s if total is None else total + s
            out.append(total)
        return jnp.concatenate(out, 1).astype(BF16)

    def attend(g, scores):
        load_v(g).wait()
        load_k(g + 1).wait()
        later = scores_of(g + 1)
        seen = seen_of(g, scores)
        term1(g, seen)

        @pl.when(g + SLOTS < groups)
        def _():
            load_v(g + SLOTS).start()

        @pl.when(g + 1 + SLOTS < groups)
        def _():
            load_k(g + 1 + SLOTS).start()

        @pl.when(g == groups - SLOTS - 1)
        def _():
            load_wg.start()

        scatter1(g)

        @pl.when((lax.rem(g, CORES) == 0) & (g >= 2 * CORES))
        def _():
            gather1(g // CORES - 2)

        return later

    load_k(0).wait()
    scores = scores_of(0)
    load_k(SLOTS).start()
    load_wo.wait()
    pl.semaphore_wait(barrier, n - 1)
    scores = lax.fori_loop(0, groups - 1, attend, scores)
    load_v(groups - 1).wait()
    term1(groups - 1, seen_of(groups - 1, scores))
    scatter1(groups - 1)
    gather1(chunks - 2)
    load_wu.start()
    gather1(chunks - 1)
    load_wd.start()

    gain_m = gm_ref[...].astype(F32)
    width = 256
    pair = 2 * cols
    pairs = chips // 2

    early = chunks - LATE
    far_pairs = ((pairs // 2, 1), (pairs - 1, 0)) if pairs > 2 else ((1,), (0,))
    partner = CORES * z + 1 - core

    def mlp(first, count, send):
        for c in range(first, first + count):
            for i in order:
                frm = peer(i)
                piece(hg.at[c, frm], hg.at[c, frm], g1s.at[c, frm], g1r.at[c, frm], frm).wait_recv()
            blocks = []
            part = jnp.zeros((CHUNK, 128), F32)
            for t in range(chips):
                block = jnp.concatenate([hg[c, CORES * t + k].astype(F32) for k in range(CORES)], 0)
                for u in range(cols // 128):
                    sub = block[:, 128 * u:128 * (u + 1)]
                    blocks.append(sub)
                    part += sub * sub
            scale = lax.rsqrt(jnp.sum(part, -1, keepdims=True) / d + 1e-6)
            for j in range(tiles):
                a16[pl.ds(c * CHUNK, CHUNK), pl.ds(128 * j, 128)] = (blocks[j] * scale * gain_m[j:j + 1]).astype(BF16)

        mine = pl.ds(first * CHUNK, count * CHUNK)
        if first == 0:
            load_wg.wait()
            load_wu.wait()

        def hidden(j, _):
            at = pl.ds(pl.multiple_of(j * width, width), width)
            b = a16[mine, :]
            gate = jnp.dot(b, wg[:, at], preferred_element_type=F32)
            up = jnp.dot(b, wu[:, at], preferred_element_type=F32)
            hb[mine, at] = (gate / (1.0 + jnp.exp(-gate)) * up).astype(BF16)
            return 0

        lax.fori_loop(0, ff // width, hidden, 0, unroll=UNROLL)
        if first == 0:
            load_wd.wait()

        b = hb[mine, :]
        for h in range(2):
            blocks = [(lax.rem(z // 2 + i, pairs), i) for i in far_pairs[h]]
            terms = [[jnp.dot(b, wd[:, pl.ds(pl.multiple_of(p * pair + o, 128), width)], preferred_element_type=F32)
                      for o in range(0, pair, width)] for p, i in blocks]
            send(h, blocks, [jnp.concatenate(t, 1).astype(BF16) for t in terms])

    def unit(term, c, k, t):
        row = c * CHUNK + half * k
        return term[row:row + half, t * cols:(t + 1) * cols]

    def scatter_late(h, blocks, terms):
        for (p, i), term in zip(blocks, terms):
            for t in range(2):
                for k in range(CORES):
                    for c in range(LATE):
                        send3[2 * CORES * p + CORES * t + k, c] = unit(term, c, k, t)
        for p, i in blocks:
            for t in range(2 * CORES):
                to = 2 * CORES * p + t
                copy = piece(send3.at[to], recv3.at[me], s2s.at[to], s2r.at[me], to)
                if i:
                    copy.start()
                else:
                    pl.when(to != me)(copy.start)

    def swap(h):
        return piece(xs2.at[h, 1 - core], xr2.at[h], xss.at[h], xsr.at[h], partner)

    def scatter_early(h, blocks, terms):
        for b, term in enumerate(terms):
            for t in range(2):
                for k in range(CORES):
                    for c in range(early):
                        xs2[h, k, 2 * b + t, c] = unit(term, c, k, t)
        swap(h).start()

    def chip_piece(h, j, t):
        return piece(sz.at[h, j], rz.at[z], zs.at[h, j], zr.at[z], CORES * t + core)

    def scatter_chips(h):
        swap(h).wait_recv()
        for b, i in enumerate(far_pairs[h]):
            for t in range(2):
                j = 2 * b + t
                sz[h, j] = (xs2[h, core, j].astype(F32) + xr2[h, j].astype(F32)).astype(BF16)
        for b, i in enumerate(far_pairs[h]):
            for t in range(2):
                to = 2 * lax.rem(z // 2 + i, pairs) + t
                copy = chip_piece(h, 2 * b + t, to)
                if i:
                    copy.start()
                else:
                    pl.when(to != z)(copy.start)

    def y_piece(t, to):
        return piece(yg.at[core, t], yg.at[core, t], ys.at[to], yr.at[t], CORES * to + core)

    def gather_early():
        for i in far[:-1]:
            t = lax.rem(z + i, chips)
            piece(rz.at[t], rz.at[t], zs.at[0, 0], zr.at[t], me).wait_recv()
        total = sz[1, 2 + lax.rem(z, 2)].astype(F32)
        for i in far[:-1]:
            total += rz[lax.rem(z + i, chips)].astype(F32)
        for c in range(early):
            yg[core, z, c] = (hg[c, me].astype(F32) + total[c]).astype(BF16)
        for i in far[:-1]:
            y_piece(z, lax.rem(z + i, chips)).start()

    def forward():
        return piece(yg.at[core], yg.at[core], fs.at[0], fr.at[0], partner)

    def forward_early():
        for i in far[:-1]:
            t = lax.rem(z + i, chips)
            y_piece(t, t).wait_recv()
        forward().start()

    def collect_early():
        forward().wait_recv()
        for c in range(early):
            for t in range(chips):
                both = jnp.concatenate([yg[k, t, c].astype(F32) for k in range(CORES)], 0)
                out_ref[pl.ds(c * CHUNK, CHUNK), pl.ds(t * cols, cols)] = both.astype(BF16)

    def gather2(first, count, send, recv, ssem, rsem, y, gsem, grsem):
        for i in order:
            frm = peer(i)
            piece(send.at[frm], recv.at[frm], ssem.at[frm], rsem.at[frm], frm).wait_recv()
        for c in range(count):
            total = send[me, c].astype(F32)
            for i in order:
                total += recv[peer(i), c].astype(F32)
            y[me, c] = (hg[first + c, me].astype(F32) + total).astype(BF16)
        for i in order:
            to = peer(i)
            piece(y.at[me], y.at[me], gsem.at[to], grsem.at[me], to).start()

    def collect2(first, count, y, gsem, grsem):
        for i in order:
            frm = peer(i)
            piece(y.at[frm], y.at[frm], gsem.at[frm], grsem.at[frm], frm).wait_recv()
        for c in range(count):
            for t in range(chips):
                both = jnp.concatenate([y[CORES * t + k, c].astype(F32) for k in range(CORES)], 0)
                out_ref[pl.ds((first + c) * CHUNK, CHUNK), pl.ds(t * cols, cols)] = both.astype(BF16)

    mlp(0, early, scatter_early)
    scatter_chips(0)
    scatter_chips(1)
    mlp(early, LATE, scatter_late)
    gather_early()
    gather2(early, LATE, send3, recv3, s2s, s2r, yh, g2s, g2r)
    forward_early()
    collect_early()
    collect2(early, LATE, yh, g2s, g2r)

    for i in order:
        to = peer(i)
        for c in range(chunks):
            piece(hg.at[c, me], hg.at[c, me], g1s.at[c, to], g1r.at[c, me], to).wait_send()
        piece(send3.at[to], send3.at[to], s2s.at[to], s2r.at[me], to).wait_send()
        piece(yh.at[me], yh.at[me], g2s.at[to], g2r.at[me], to).wait_send()
    for h in range(2):
        swap(h).wait_send()
        for b, i in enumerate(far_pairs[h]):
            for t in range(2):
                to = 2 * lax.rem(z // 2 + i, pairs) + t
                copy = chip_piece(h, 2 * b + t, to)
                if i:
                    copy.wait_send()
                else:
                    pl.when(to != z)(copy.wait_send)
    for i in far[:-1]:
        y_piece(z, lax.rem(z + i, chips)).wait_send()
    forward().wait_send()
    for u in range(groups):
        for i in far:
            t = lax.rem(z + i, chips)
            copy = piece(send1.at[u, t], send1.at[u, t], s1s.at[u, t], s1r.at[u // CORES, me], me)
            if i:
                copy.wait_send()
            else:
                pl.when(core != u % CORES)(copy.wait_send)


def solution(mesh):
    n = mesh.shape["tp"]

    def step(x, k_cache, v_cache, gain_a, wq, wo, gain_m, w_gate, w_up, w_down):
        rows, d = x.shape
        cache = k_cache.shape[1]
        ff = w_gate.shape[1]
        k_cache, v_cache = k_cache.reshape(rows, cache, HEAD), v_cache.reshape(rows, cache, HEAD)
        chunks, half, cols = rows // CHUNK, CHUNK // CORES, d // (n // CORES)
        early = (chunks - LATE, half, cols)
        trig = jnp.asarray(rotary_table(cache, HEAD // 2))
        any_, vmem = pl.BlockSpec(memory_space=pl.ANY), pl.BlockSpec(memory_space=pltpu.VMEM)
        dma = pltpu.SemaphoreType.DMA
        return pl.pallas_call(
            functools.partial(layer, n),
            name="layer",
            out_shape=pltpu.VMEM((rows, d), BF16),
            in_specs=[any_, any_, any_, vmem, vmem, any_, any_, vmem, any_, any_, any_],
            out_specs=vmem,
            scratch_shapes=[
                pltpu.VMEM((rows, d), BF16),
                pltpu.VMEM((rows, d), F32),
                pltpu.VMEM((rows, d), BF16),
                pltpu.VMEM(wq.shape, BF16),
                pltpu.VMEM(wo.shape, BF16),
                pltpu.VMEM(w_gate.shape, BF16),
                pltpu.VMEM(w_up.shape, BF16),
                pltpu.VMEM(w_down.shape, BF16),
                pltpu.VMEM((SLOTS, GROUP, cache, HEAD), BF16),
                pltpu.VMEM((SLOTS, GROUP, cache, HEAD), BF16),
                pltpu.VMEM((rows, HEAD), F32),
                pltpu.VMEM((rows, ff), BF16),
                pltpu.VMEM((rows // GROUP, n // CORES, half, cols), BF16),
                pltpu.VMEM((chunks, n, half, cols), BF16),
                pltpu.VMEM((chunks, n, half, cols), BF16),
                pltpu.VMEM((2, CORES, n // CORES // 2, *early), BF16),
                pltpu.VMEM((2, n // CORES // 2, *early), BF16),
                pltpu.VMEM((2, n // CORES // 2, *early), BF16),
                pltpu.VMEM((n // CORES, *early), BF16),
                pltpu.VMEM((CORES, n // CORES, *early), BF16),
                *[pltpu.VMEM((n, LATE, half, cols), BF16)] * 3,
                dma((6,)),
                dma((SLOTS,)),
                dma((SLOTS,)),
                dma((rows // GROUP, n // CORES)),
                dma((chunks, n)),
                dma((chunks, n)),
                dma((chunks, n)),
                *[dma((n,))] * 4,
                *[dma((2,))] * 2,
                dma((2, n // CORES // 2)),
                *[dma((n // CORES,))] * 3,
                *[dma((1,))] * 2,
            ],
            compiler_params=pltpu.CompilerParams(
                collective_id=0, has_side_effects=True, vmem_limit_bytes=60 * 1024 * 1024
            ),
        )(x, k_cache, v_cache, gain_a.reshape(-1, 128), trig, wq, wo, gain_m.reshape(-1, 128), w_gate, w_up, w_down)

    states, cache, columns, rows_of = P("dp", None), P("dp", None, "tp", None), P(None, "tp"), P("tp", None)
    return jax.shard_map(
        step,
        mesh=mesh,
        in_specs=(states, cache, cache, P(None), columns, rows_of, P(None), columns, columns, rows_of),
        out_specs=states,
        check_vma=False,
    )
```

```python
import functools

import jax
import jax.numpy as jnp
import numpy as np
from jax import lax
from jax.experimental import pallas as pl
from jax.experimental.pallas import tpu as pltpu
from jax.sharding import PartitionSpec as P

HEAD = 256
THETA = 10000
CORES = 2
GROUP = 8
CHUNK = 16
SLOTS = 3
LATE = 1
UNROLL = True
MESH = pl.DeviceIdType.MESH
F32, BF16 = jnp.float32, jnp.bfloat16


def rotary_table(cache, half):
    angle = np.float32(cache - 1) * (np.float32(THETA) ** (-np.arange(half, dtype=np.float32) / half))
    return np.stack([np.cos(angle), np.sin(angle)]).astype(np.float32)


def layer(n, x_hbm, k_hbm, v_hbm, ga_ref, trig_ref, wq_hbm, wo_hbm, gm_ref, wg_hbm, wu_hbm, wd_hbm, out_ref,
          x16, xs, a16, wq, wo, wg, wu, wd, kbuf, vbuf, q32, hb,
          send1, recv1, hg, xs2, xr2, sz, rz, yg, send3, recv3, yh,
          in_sem, k_sem, v_sem, s1s, s1r, g1s, g1r, s2s, s2r, g2s, g2r, xss, xsr, zs, zr, ys, yr, fs, fr):
    rows, d = x16.shape
    ff = wg.shape[1]
    groups, chunks = rows // GROUP, rows // CHUNK
    half = CHUNK // CORES
    chips = n // CORES
    cols = d // chips
    me = lax.axis_index("tp")
    z, core = me // CORES, lax.rem(me, CORES)
    tiles = d // 128

    def peer(i):
        return lax.rem(me + i, n)

    order = sorted(range(1, n), key=lambda i: -min(i, n - i))
    far = [chips // 2]
    for i in range(chips // 2 - 1, 0, -1):
        far += [i, chips - i]
    far.append(0)

    load_x = pltpu.make_async_copy(x_hbm, x16, in_sem.at[0])
    load_wq = pltpu.make_async_copy(wq_hbm, wq, in_sem.at[1])
    load_wo = pltpu.make_async_copy(wo_hbm, wo, in_sem.at[2])
    load_wg = pltpu.make_async_copy(wg_hbm, wg, in_sem.at[3])
    top = pl.ds(0, d // 2)
    bottom = pl.ds(d // 2, d // 2)
    load_wu = pltpu.make_async_copy(wu_hbm.at[top], wu.at[top], in_sem.at[4])
    load_wu2 = pltpu.make_async_copy(wu_hbm.at[bottom], wu.at[bottom], in_sem.at[6])
    load_wd = pltpu.make_async_copy(wd_hbm, wd, in_sem.at[5])

    def load_k(g):
        slot = lax.rem(g, SLOTS)
        return pltpu.make_async_copy(k_hbm.at[pl.ds(g * GROUP, GROUP)], kbuf.at[slot], k_sem.at[slot])

    def load_v(g):
        slot = lax.rem(g, SLOTS)
        return pltpu.make_async_copy(v_hbm.at[pl.ds(g * GROUP, GROUP)], vbuf.at[slot], v_sem.at[slot])

    load_x.start()
    load_wq.start()
    for g in range(SLOTS):
        load_k(g).start()
        load_v(g).start()
        if g == 0:
            load_wo.start()

    barrier = pltpu.get_barrier_semaphore()
    for i in range(1, n):
        pl.semaphore_signal(barrier, inc=1, device_id={"tp": peer(i)}, device_id_type=MESH)

    load_x.wait()
    part = jnp.zeros((rows, 128), F32)
    for j in range(tiles):
        block = x16[:, pl.ds(128 * j, 128)].astype(F32)
        xs[:, pl.ds(128 * j, 128)] = block
        part += block * block
    scale = lax.rsqrt(jnp.sum(part, -1, keepdims=True) / d + 1e-6)
    gain = ga_ref[...].astype(F32)
    for j in range(tiles):
        a16[:, pl.ds(128 * j, 128)] = (xs[:, pl.ds(128 * j, 128)] * scale * gain[j:j + 1]).astype(BF16)
    load_wq.wait()
    q = [jnp.dot(a16[...], wq[:, pl.ds(o, 128)], preferred_element_type=F32).astype(BF16).astype(F32) for o in range(0, HEAD, 128)]
    q = jnp.concatenate(q, 1)
    turn = HEAD // 2
    cos, sin = trig_ref[0:1], trig_ref[1:2]
    qa, qb = q[:, :turn], q[:, turn:]
    q32[:, :turn] = (qa * cos - qb * sin).astype(BF16).astype(F32)
    q32[:, turn:] = (qb * cos + qa * sin).astype(BF16).astype(F32)

    def piece(src, dst, ssem, rsem, to):
        return pltpu.make_async_remote_copy(src_ref=src, dst_ref=dst, send_sem=ssem, recv_sem=rsem,
                                            device_id={"tp": to}, device_id_type=MESH)

    def term1(u, seen):
        term = jnp.concatenate([jnp.dot(seen, wo[:, pl.ds(o, 256)], preferred_element_type=F32) for o in range(0, d, 256)], 1)
        for t in range(chips):
            send1[u, t] = term[:, t * cols:(t + 1) * cols].astype(BF16)

    def scatter1(u):
        kind = lax.rem(u, CORES)
        c = u // CORES
        for i in far:
            t = lax.rem(z + i, chips)
            to = CORES * t + kind
            copy = piece(send1.at[u, t], recv1.at[c, me], s1s.at[u, t], s1r.at[c, me], to)
            if i:
                copy.start()
            else:
                pl.when(core != kind)(copy.start)

    def gather1(c):
        u = CORES * c + core
        total = send1[u, z].astype(F32)
        for i in order:
            frm = peer(i)
            piece(send1.at[u, z], recv1.at[c, frm], s1s.at[u, z], s1r.at[c, frm], frm).wait_recv()
        for i in order:
            total += recv1[c, peer(i)].astype(F32)
        at = pl.ds(pl.multiple_of(u * half, half), half)
        hg[c, me] = (xs[at, pl.ds(pl.multiple_of(z * cols, 128), cols)] + total).astype(BF16)
        for i in order:
            to = peer(i)
            piece(hg.at[c, me], hg.at[c, me], g1s.at[c, to], g1r.at[c, me], to).start()

    line = lax.broadcasted_iota(jnp.int32, (GROUP, 1), 0)

    def scores_of(g):
        slot = lax.rem(g, SLOTS)
        qg = q32[pl.ds(pl.multiple_of(g * GROUP, GROUP), GROUP), :]
        lhs = [jnp.where(line == i, qg, 0.0).astype(BF16) for i in range(GROUP)]
        out = []
        for j in range(kbuf.shape[2] // 256):
            total = None
            for i in range(GROUP):
                s = lax.dot_general(lhs[i], kbuf[slot, i, pl.ds(256 * j, 256)], (((1,), (1,)), ((), ())), preferred_element_type=F32)
                total = s if total is None else total + s
            out.append(total)
        return jnp.concatenate(out, 1) * HEAD**-0.5

    def seen_of(g, scores):
        slot = lax.rem(g, SLOTS)
        e = jnp.exp(scores - jnp.max(scores, -1, keepdims=True))
        w = e * (1.0 / jnp.sum(e, -1, keepdims=True))
        lhs = [jnp.where(line == i, w, 0.0).astype(BF16) for i in range(GROUP)]
        out = []
        for j in range(HEAD // 128):
            total = None
            for i in range(GROUP):
                s = jnp.dot(lhs[i], vbuf[slot, i, :, pl.ds(128 * j, 128)], preferred_element_type=F32)
                total = s if total is None else total + s
            out.append(total)
        return jnp.concatenate(out, 1).astype(BF16)

    def attend(g, scores):
        load_v(g).wait()
        load_k(g + 1).wait()
        later = scores_of(g + 1)
        seen = seen_of(g, scores)
        term1(g, seen)

        scatter1(g)

        @pl.when(g + SLOTS < groups)
        def _():
            load_v(g + SLOTS).start()

        @pl.when(g + 1 + SLOTS < groups)
        def _():
            load_k(g + 1 + SLOTS).start()

        @pl.when(g == groups - SLOTS - 1)
        def _():
            load_wg.start()
            load_wu.start()

        @pl.when((lax.rem(g, CORES) == 0) & (g >= 2 * CORES))
        def _():
            gather1(g // CORES - 2)

        return later

    load_k(0).wait()
    scores = scores_of(0)
    load_k(SLOTS).start()
    load_wo.wait()
    pl.semaphore_wait(barrier, n - 1)
    scores = lax.fori_loop(0, groups - 1, attend, scores)
    load_v(groups - 1).wait()
    term1(groups - 1, seen_of(groups - 1, scores))
    scatter1(groups - 1)
    gather1(chunks - 2)
    load_wu2.start()
    gather1(chunks - 1)
    load_wd.start()

    gain_m = gm_ref[...].astype(F32)
    width = 256
    pair = 2 * cols
    pairs = chips // 2

    early = chunks - LATE
    far_pairs = ((pairs // 2, 1), (pairs - 1, 0)) if pairs > 2 else ((1,), (0,))
    partner = CORES * z + 1 - core

    def mlp(first, count, send):
        for c in range(first, first + count):
            for i in order:
                frm = peer(i)
                piece(hg.at[c, frm], hg.at[c, frm], g1s.at[c, frm], g1r.at[c, frm], frm).wait_recv()
            blocks = []
            part = jnp.zeros((CHUNK, 128), F32)
            for t in range(chips):
                block = jnp.concatenate([hg[c, CORES * t + k].astype(F32) for k in range(CORES)], 0)
                for u in range(cols // 128):
                    sub = block[:, 128 * u:128 * (u + 1)]
                    blocks.append(sub)
                    part += sub * sub
            scale = lax.rsqrt(jnp.sum(part, -1, keepdims=True) / d + 1e-6)
            for j in range(tiles):
                a16[pl.ds(c * CHUNK, CHUNK), pl.ds(128 * j, 128)] = (blocks[j] * scale * gain_m[j:j + 1]).astype(BF16)

        mine = pl.ds(first * CHUNK, count * CHUNK)
        if first == 0:
            load_wg.wait()
            load_wu.wait()
            load_wu2.wait()

        def hidden(j, _):
            at = pl.ds(pl.multiple_of(j * width, width), width)
            b = a16[mine, :]
            gate = jnp.dot(b, wg[:, at], preferred_element_type=F32)
            up = jnp.dot(b, wu[:, at], preferred_element_type=F32)
            hb[mine, at] = (gate / (1.0 + jnp.exp(-gate)) * up).astype(BF16)
            return 0

        lax.fori_loop(0, ff // width, hidden, 0, unroll=UNROLL)
        if first == 0:
            load_wd.wait()

        b = hb[mine, :]
        for h in range(2):
            blocks = [(lax.rem(z // 2 + i, pairs), i) for i in far_pairs[h]]
            terms = [[jnp.dot(b, wd[:, pl.ds(pl.multiple_of(p * pair + o, 128), width)], preferred_element_type=F32)
                      for o in range(0, pair, width)] for p, i in blocks]
            send(h, blocks, [jnp.concatenate(t, 1).astype(BF16) for t in terms])

    def unit(term, c, k, t):
        row = c * CHUNK + half * k
        return term[row:row + half, t * cols:(t + 1) * cols]

    def scatter_late(h, blocks, terms):
        for (p, i), term in zip(blocks, terms):
            for t in range(2):
                for k in range(CORES):
                    for c in range(LATE):
                        send3[2 * CORES * p + CORES * t + k, c] = unit(term, c, k, t)
        for p, i in blocks:
            for t in range(2 * CORES):
                to = 2 * CORES * p + t
                copy = piece(send3.at[to], recv3.at[me], s2s.at[to], s2r.at[me], to)
                if i:
                    copy.start()
                else:
                    pl.when(to != me)(copy.start)

    def swap(h):
        return piece(xs2.at[h, 1 - core], xr2.at[h], xss.at[h], xsr.at[h], partner)

    def scatter_early(h, blocks, terms):
        for b, term in enumerate(terms):
            for t in range(2):
                for k in range(CORES):
                    for c in range(early):
                        xs2[h, k, 2 * b + t, c] = unit(term, c, k, t)
        swap(h).start()

    def chip_piece(h, j, t):
        return piece(sz.at[h, j], rz.at[z], zs.at[h, j], zr.at[z], CORES * t + core)

    def scatter_chips(h):
        swap(h).wait_recv()
        for b, i in enumerate(far_pairs[h]):
            for t in range(2):
                j = 2 * b + t
                sz[h, j] = (xs2[h, core, j].astype(F32) + xr2[h, j].astype(F32)).astype(BF16)
        for b, i in enumerate(far_pairs[h]):
            for t in range(2):
                to = 2 * lax.rem(z // 2 + i, pairs) + t
                copy = chip_piece(h, 2 * b + t, to)
                if i:
                    copy.start()
                else:
                    pl.when(to != z)(copy.start)

    def y_piece(t, to):
        return piece(yg.at[core, t], yg.at[core, t], ys.at[to], yr.at[t], CORES * to + core)

    def gather_early():
        for i in far[:-1]:
            t = lax.rem(z + i, chips)
            piece(rz.at[t], rz.at[t], zs.at[0, 0], zr.at[t], me).wait_recv()
        total = sz[1, 2 + lax.rem(z, 2)].astype(F32)
        for i in far[:-1]:
            total += rz[lax.rem(z + i, chips)].astype(F32)
        for c in range(early):
            yg[core, z, c] = (hg[c, me].astype(F32) + total[c]).astype(BF16)
        for i in far[:-1]:
            y_piece(z, lax.rem(z + i, chips)).start()

    def forward():
        return piece(yg.at[core], yg.at[core], fs.at[0], fr.at[0], partner)

    def forward_early():
        for i in far[:-1]:
            t = lax.rem(z + i, chips)
            y_piece(t, t).wait_recv()
        forward().start()

    def collect_early():
        forward().wait_recv()
        for c in range(early):
            for t in range(chips):
                both = jnp.concatenate([yg[k, t, c].astype(F32) for k in range(CORES)], 0)
                out_ref[pl.ds(c * CHUNK, CHUNK), pl.ds(t * cols, cols)] = both.astype(BF16)

    def gather2(first, count, send, recv, ssem, rsem, y, gsem, grsem):
        for i in order:
            frm = peer(i)
            piece(send.at[frm], recv.at[frm], ssem.at[frm], rsem.at[frm], frm).wait_recv()
        for c in range(count):
            total = send[me, c].astype(F32)
            for i in order:
                total += recv[peer(i), c].astype(F32)
            y[me, c] = (hg[first + c, me].astype(F32) + total).astype(BF16)
        for i in order:
            to = peer(i)
            piece(y.at[me], y.at[me], gsem.at[to], grsem.at[me], to).start()

    def collect2(first, count, y, gsem, grsem):
        for i in order:
            frm = peer(i)
            piece(y.at[frm], y.at[frm], gsem.at[frm], grsem.at[frm], frm).wait_recv()
        for c in range(count):
            for t in range(chips):
                both = jnp.concatenate([y[CORES * t + k, c].astype(F32) for k in range(CORES)], 0)
                out_ref[pl.ds((first + c) * CHUNK, CHUNK), pl.ds(t * cols, cols)] = both.astype(BF16)

    mlp(0, early, scatter_early)
    scatter_chips(0)
    scatter_chips(1)
    mlp(early, LATE, scatter_late)
    gather_early()
    gather2(early, LATE, send3, recv3, s2s, s2r, yh, g2s, g2r)
    forward_early()
    collect_early()
    collect2(early, LATE, yh, g2s, g2r)

    for i in order:
        to = peer(i)
        for c in range(chunks):
            piece(hg.at[c, me], hg.at[c, me], g1s.at[c, to], g1r.at[c, me], to).wait_send()
        piece(send3.at[to], send3.at[to], s2s.at[to], s2r.at[me], to).wait_send()
        piece(yh.at[me], yh.at[me], g2s.at[to], g2r.at[me], to).wait_send()
    for h in range(2):
        swap(h).wait_send()
        for b, i in enumerate(far_pairs[h]):
            for t in range(2):
                to = 2 * lax.rem(z // 2 + i, pairs) + t
                copy = chip_piece(h, 2 * b + t, to)
                if i:
                    copy.wait_send()
                else:
                    pl.when(to != z)(copy.wait_send)
    for i in far[:-1]:
        y_piece(z, lax.rem(z + i, chips)).wait_send()
    forward().wait_send()
    for u in range(groups):
        for i in far:
            t = lax.rem(z + i, chips)
            copy = piece(send1.at[u, t], send1.at[u, t], s1s.at[u, t], s1r.at[u // CORES, me], me)
            if i:
                copy.wait_send()
            else:
                pl.when(core != u % CORES)(copy.wait_send)


def solution(mesh):
    n = mesh.shape["tp"]

    def step(x, k_cache, v_cache, gain_a, wq, wo, gain_m, w_gate, w_up, w_down):
        rows, d = x.shape
        cache = k_cache.shape[1]
        ff = w_gate.shape[1]
        k_cache, v_cache = k_cache.reshape(rows, cache, HEAD), v_cache.reshape(rows, cache, HEAD)
        chunks, half, cols = rows // CHUNK, CHUNK // CORES, d // (n // CORES)
        early = (chunks - LATE, half, cols)
        trig = jnp.asarray(rotary_table(cache, HEAD // 2))
        any_, vmem = pl.BlockSpec(memory_space=pl.ANY), pl.BlockSpec(memory_space=pltpu.VMEM)
        dma = pltpu.SemaphoreType.DMA
        return pl.pallas_call(
            functools.partial(layer, n),
            name="layer",
            out_shape=pltpu.VMEM((rows, d), BF16),
            in_specs=[any_, any_, any_, vmem, vmem, any_, any_, vmem, any_, any_, any_],
            out_specs=vmem,
            scratch_shapes=[
                pltpu.VMEM((rows, d), BF16),
                pltpu.VMEM((rows, d), F32),
                pltpu.VMEM((rows, d), BF16),
                pltpu.VMEM(wq.shape, BF16),
                pltpu.VMEM(wo.shape, BF16),
                pltpu.VMEM(w_gate.shape, BF16),
                pltpu.VMEM(w_up.shape, BF16),
                pltpu.VMEM(w_down.shape, BF16),
                pltpu.VMEM((SLOTS, GROUP, cache, HEAD), BF16),
                pltpu.VMEM((SLOTS, GROUP, cache, HEAD), BF16),
                pltpu.VMEM((rows, HEAD), F32),
                pltpu.VMEM((rows, ff), BF16),
                pltpu.VMEM((rows // GROUP, n // CORES, half, cols), BF16),
                pltpu.VMEM((chunks, n, half, cols), BF16),
                pltpu.VMEM((chunks, n, half, cols), BF16),
                pltpu.VMEM((2, CORES, n // CORES // 2, *early), BF16),
                pltpu.VMEM((2, n // CORES // 2, *early), BF16),
                pltpu.VMEM((2, n // CORES // 2, *early), BF16),
                pltpu.VMEM((n // CORES, *early), BF16),
                pltpu.VMEM((CORES, n // CORES, *early), BF16),
                *[pltpu.VMEM((n, LATE, half, cols), BF16)] * 3,
                dma((7,)),
                dma((SLOTS,)),
                dma((SLOTS,)),
                dma((rows // GROUP, n // CORES)),
                dma((chunks, n)),
                dma((chunks, n)),
                dma((chunks, n)),
                *[dma((n,))] * 4,
                *[dma((2,))] * 2,
                dma((2, n // CORES // 2)),
                *[dma((n // CORES,))] * 3,
                *[dma((1,))] * 2,
            ],
            compiler_params=pltpu.CompilerParams(
                collective_id=0, has_side_effects=True, vmem_limit_bytes=60 * 1024 * 1024
            ),
        )(x, k_cache, v_cache, gain_a.reshape(-1, 128), trig, wq, wo, gain_m.reshape(-1, 128), w_gate, w_up, w_down)

    states, cache, columns, rows_of = P("dp", None), P("dp", None, "tp", None), P(None, "tp"), P("tp", None)
    return jax.shard_map(
        step,
        mesh=mesh,
        in_specs=(states, cache, cache, P(None), columns, rows_of, P(None), columns, columns, rows_of),
        out_specs=states,
        check_vma=False,
    )
```
